256 devices in a mesh: sy: 16 (over y, x), sx: 8 (over z), wl: 2 (over core).
Axes of the slice: x: 4, y: 4, z: 8, core: 2. Of those that a mesh axis runs over, the one named last changes fastest.
Arguments:
- interface_map: bfloat16 [32, 8, 1536, 2, 1536], P(('wl', 'sy'), 'sx'), parts along dimension 0, may hold values from -0.0625 to 0.0625
- source_trace: float32 [32, 8, 2, 64, 4, 384], P(('wl', 'sy'), 'sx'), parts along dimension 0, may hold values from -6 to 6
- restriction: float32 [32, 8, 2, 32, 4, 384], P(('wl', 'sy'), 'sx'), parts along dimension 0, may hold values from -0.009765625 to 0.009765625
- prolongation: float32 [32, 8, 2, 32, 4, 384], P(('wl', 'sy'), 'sx'), parts along dimension 0, may hold values from -0.109375 to 0.109375
- coarse_inverse: float32 [4, 32, 32], P('wl'), parts along dimension 0, may hold values from -0.75 to 0.75
Outputs:
- traces: float32 [32, 8, 2, 64, 4, 384], P(('wl', 'sy'), 'sx'), parts along dimension 0
- coarse_coef: float32 [4, 64, 32], P('wl'), parts along dimension 0
The draws below stay inside these ranges and needn't reach their ends.
There are 2 independent parts, one for each index of `wl`. The reference program is written for one: setup_inputs(seed, part) draws one part's arguments, and reference() takes and returns one part's arrays. A program takes and returns all parts, laid end to end along the dimension named above; each array names one. Nothing has to cross between parts.
All inputs are finite; a program needn't handle non-finite values.
Results may differ from the reference program's by a relative error of at most 0.0025.
Values sent between devices are 32-bit elements; how exact they have to be, the bound alone decides.
A program may use at most 128 MiB of HBM per device.

```python
import jax
import jax.numpy as jnp
from jax import lax

M = 384
NC = 32
S = 64
ITERS = 6
SUBY = 16
SUBX = 8


def steps_of(stream_key, extent, cuts, low, top_value):
    loudness, own = 1.0, jax.random.fold_in(stream_key, 6)
    for position, parts in cuts:
        draws = jnp.exp(jax.random.uniform(jax.random.fold_in(own, position), (parts,), jnp.float32, low / len(cuts), top_value / len(cuts)))
        loudness = loudness * jnp.repeat(draws, extent[position] // parts).reshape([-1 if axis == position else 1 for axis in range(len(extent))])
    return loudness


def centred(key, extent, width, most, cuts=(), dtype=jnp.bfloat16):
    drawn = jax.random.normal(key, extent, jnp.float32) * width
    if len(cuts) > 0:
        drawn = steps_of(key, extent, cuts, -0.22, 0.18) * drawn
    return jnp.clip(drawn, min=-most, max=most).astype(dtype)


def setup_inputs(seed: int = 0, part: int = 0) -> dict:
    key_list = jax.random.split(jax.random.key(seed), 6)
    own_keys = jax.random.split(jax.random.fold_in(key_list[5], part), 6)
    return {
        "interface_map": centred(own_keys[0], (SUBY, SUBX, 4 * M, 2, 4 * M), (24 * M) ** -0.5, 0.0625, ((0, 16), (1, 8))),
        "source_trace": centred(own_keys[1], (SUBY, SUBX, 2, S, 4, M), 1.0, 6.0, ((0, 16), (1, 8)), jnp.float32),
        "restriction": centred(own_keys[2], (SUBY, SUBX, 2, NC, 4, M), (8 * M * SUBY * SUBX) ** -0.5, 0.009765625, ((0, 16), (1, 8)), jnp.float32),
        "prolongation": centred(own_keys[3], (SUBY, SUBX, 2, NC, 4, M), (96 * NC) ** -0.5, 0.109375, ((0, 16), (1, 8)), jnp.float32),
        "coarse_inverse": centred(own_keys[4], (2, NC, NC), (2 * NC) ** -0.5, 0.75, (), jnp.float32),
    }


PRECISE = lax.Precision.HIGHEST


def shifted(values, along, offset):
    length_axis = values.shape[along]
    blank_edge = jnp.zeros_like(lax.slice_in_dim(values, 0, 1, axis=along))
    if offset == 1:
        return jnp.concatenate([blank_edge, lax.slice_in_dim(values, 0, length_axis - 1, axis=along)], axis=along)
    return jnp.concatenate([lax.slice_in_dim(values, 1, length_axis, axis=along), blank_edge], axis=along)


def complex_pair(left_real, left_imag, right_real, right_imag, pattern):
    real_part = jnp.einsum(pattern, left_real, right_real, precision=PRECISE) - jnp.einsum(pattern, left_imag, right_imag, precision=PRECISE)
    imag_part = jnp.einsum(pattern, left_real, right_imag, precision=PRECISE) + jnp.einsum(pattern, left_imag, right_real, precision=PRECISE)
    return jnp.stack([real_part, imag_part])


def corner_values(outgoing):
    corner_northwest = outgoing[..., 0, 0] + outgoing[..., 2, 0]
    corner_northeast = outgoing[..., 0, -1] + outgoing[..., 3, 0]
    corner_southwest = outgoing[..., 1, 0] + outgoing[..., 2, -1]
    corner_southeast = outgoing[..., 1, -1] + outgoing[..., 3, -1]
    return corner_northwest, corner_northeast, corner_southwest, corner_southeast


def assemble(from_north, from_south, from_west, from_east, into_northwest, into_northeast, into_southwest, into_southeast):
    north_side = from_north.at[..., 0].add(0.5 * into_northwest).at[..., -1].add(0.5 * into_northeast)
    south_side = from_south.at[..., 0].add(0.5 * into_southwest).at[..., -1].add(0.5 * into_southeast)
    west_side = from_west.at[..., 0].add(0.5 * into_northwest).at[..., -1].add(0.5 * into_southwest)
    east_side = from_east.at[..., 0].add(0.5 * into_northeast).at[..., -1].add(0.5 * into_southeast)
    return jnp.stack([north_side, south_side, west_side, east_side], axis=-2)


def reference(interface_map, source_trace, restriction, prolongation, coarse_inverse):
    grid_rows, grid_cols = source_trace.shape[0], source_trace.shape[1]
    src_count, side_len = source_trace.shape[3], source_trace.shape[5]
    coarse_width = restriction.shape[3]
    flat_map = interface_map.reshape(grid_rows * grid_cols, 4 * side_len, 8 * side_len)
    rest_flat = restriction.reshape(grid_rows, grid_cols, 2, coarse_width, 4 * side_len)
    lift_flat = prolongation.reshape(grid_rows, grid_cols, 2, coarse_width, 4 * side_len)
    traces = jnp.zeros(source_trace.shape, jnp.float32)
    coef_now = jnp.zeros((2, src_count, coarse_width), jnp.float32)
    for sweep_index in range(ITERS):
        flat_traces = traces.reshape(grid_rows, grid_cols, 2, src_count, 4 * side_len)
        coarse_total = complex_pair(flat_traces[:, :, 0], flat_traces[:, :, 1], rest_flat[:, :, 0], rest_flat[:, :, 1], "yxsk,yxnk->sn")
        coef_now = complex_pair(coarse_total[0], coarse_total[1], coarse_inverse[0], coarse_inverse[1], "sn,nq->sq")
        spread = complex_pair(coef_now[0], coef_now[1], lift_flat[:, :, 0], lift_flat[:, :, 1], "sn,yxnk->yxsk")
        corrected = flat_traces + jnp.moveaxis(spread, 0, 2)
        row_block = corrected.astype(jnp.bfloat16).reshape(grid_rows * grid_cols, 2 * src_count, 4 * side_len)
        product = lax.map(lambda operands: jnp.dot(operands[0], operands[1], preferred_element_type=jnp.float32), (row_block, flat_map))
        product = product.reshape(grid_rows, grid_cols, 2, src_count, 2, 4 * side_len)
        real_part = product[:, :, 0, :, 0] - product[:, :, 1, :, 1]
        imag_part = product[:, :, 0, :, 1] + product[:, :, 1, :, 0]
        outgoing = jnp.stack([real_part, imag_part], axis=2).reshape(source_trace.shape) + source_trace
        from_north = shifted(outgoing[:, :, :, :, 1], 0, 1)
        from_south = shifted(outgoing[:, :, :, :, 0], 0, -1)
        from_west = shifted(outgoing[:, :, :, :, 3], 1, 1)
        from_east = shifted(outgoing[:, :, :, :, 2], 1, -1)
        corner_northwest, corner_northeast, corner_southwest, corner_southeast = corner_values(outgoing)
        into_northwest = shifted(shifted(corner_southeast, 0, 1), 1, 1)
        into_northeast = shifted(shifted(corner_southwest, 0, 1), 1, -1)
        into_southwest = shifted(shifted(corner_northeast, 0, -1), 1, 1)
        into_southeast = shifted(shifted(corner_northwest, 0, -1), 1, -1)
        traces = assemble(from_north, from_south, from_west, from_east, into_northwest, into_northeast, into_southwest, into_southeast)
    return traces, coef_now
```

```python
import functools

import jax
import jax.numpy as jnp
from jax import lax
from jax.experimental import pallas as pl
from jax.experimental.pallas import tpu as pltpu
from jax.sharding import PartitionSpec as P

ITERS = 6
LANES = 128
MESH = pl.DeviceIdType.MESH
HIGH = lax.Precision.HIGHEST
NORTH, SOUTH, WEST, EAST = 0, 1, 2, 3
OUT_OF = {NORTH: SOUTH, SOUTH: NORTH, WEST: EAST, EAST: WEST}


def dot(a, b, contract, precision=None):
    return lax.dot_general(
        a, b, (contract, ((), ())), preferred_element_type=jnp.float32, precision=precision
    )


def turned(pair, half):
    return jnp.concatenate([-pair[:, half:], pair[:, :half]], axis=1)


def kernel(
    dims,
    map_hbm,
    src_ref,
    res_ref,
    pro_ref,
    inv_ref,
    out_ref,
    coef_ref,
    table,
    lhs,
    low,
    sent,
    got,
    lift,
    res_split,
    corner_out,
    corner_in,
    part,
    plane_in,
    line_out,
    line_in,
    col_out,
    col_in,
    fix,
    map_sem,
    send_sem,
    recv_sem,
    csend_sem,
    crecv_sem,
    asend_sem,
    arecv_sem,
):
    ny, nx, nz, s2, q2, thirds = dims
    cells = thirds * LANES
    nsy = ny * nx
    rows_all = s2 + q2
    half_s, half_q = s2 // 2, q2 // 2
    sy, sx = lax.axis_index("sy"), lax.axis_index("sx")
    wl = lax.axis_index("wl")
    yy = sy // nx

    def dev(row, col):
        return (row, col, wl)

    up, down = lax.rem(sy + nsy - 1, nsy), lax.rem(sy + 1, nsy)
    left, right = lax.rem(sx + nz - 1, nz), lax.rem(sx + 1, nz)
    peer = {NORTH: dev(up, sx), SOUTH: dev(down, sx), WEST: dev(sy, left), EAST: dev(sy, right)}
    diag = (dev(up, left), dev(up, right), dev(down, left), dev(down, right))
    has = {NORTH: sy > 0, SOUTH: sy < nsy - 1, WEST: sx > 0, EAST: sx < nz - 1}
    has_diag = (
        (sy > 0) & (sx > 0),
        (sy > 0) & (sx < nz - 1),
        (sy < nsy - 1) & (sx > 0),
        (sy < nsy - 1) & (sx < nz - 1),
    )

    loads = [
        [pltpu.make_async_copy(map_hbm.at[t, h], table.at[t, h], map_sem.at[t, h]) for h in (0, 1)]
        for t in range(thirds)
    ]
    order = (0, *range(2, thirds), 1)
    for t in order:
        for h in (0, 1):
            loads[t][h].start()

    barrier = pltpu.get_barrier_semaphore()
    met = 0
    for target in (*peer.values(), *diag):
        pl.semaphore_signal(barrier, inc=1, device_id=target, device_id_type=MESH)
        met += 1
    for d in range(1, nsy):
        target = dev(lax.rem(sy + d, nsy), sx)
        pl.semaphore_signal(barrier, inc=1, device_id=target, device_id_type=MESH)
        met += 1
    for d in range(1, nz):
        target = dev(sy, lax.rem(sx + d, nz))
        pl.semaphore_signal(barrier, inc=1, device_id=target, device_id_type=MESH)
        met += 1
    pl.semaphore_wait(barrier, met)

    lane = lax.broadcasted_iota(jnp.int32, (1, LANES), 1)

    def rows_of(e):
        return rows_all if e in (2, 3) else s2

    def side_copy(e, side, t):
        par, rows = e % 2, rows_of(e)
        src = src_ref.at[side, t] if e == 1 else sent.at[side, t, pl.ds(0, rows)]
        return pltpu.make_async_remote_copy(
            src_ref=src,
            dst_ref=got.at[par, OUT_OF[side], t, pl.ds(0, rows)],
            send_sem=send_sem.at[side, t],
            recv_sem=recv_sem.at[par, OUT_OF[side], t],
            device_id=peer[side],
            device_id_type=MESH,
        )

    def corner_copy(e, k):
        par = e % 2
        return pltpu.make_async_remote_copy(
            src_ref=corner_out.at[par],
            dst_ref=corner_in.at[par, 3 - k],
            send_sem=csend_sem.at[par, k],
            recv_sem=crecv_sem.at[par, 3 - k],
            device_id=diag[k],
            device_id_type=MESH,
        )

    def send_corners(e, block):
        last = thirds - 1
        n0, n1 = block(NORTH, 0)[:, 0:1], block(NORTH, last)[:, LANES - 1 :]
        s0, s1 = block(SOUTH, 0)[:, 0:1], block(SOUTH, last)[:, LANES - 1 :]
        w0, w1 = block(WEST, 0)[:, 0:1], block(WEST, last)[:, LANES - 1 :]
        e0, e1 = block(EAST, 0)[:, 0:1], block(EAST, last)[:, LANES - 1 :]
        nw, ne, sw, se = n0 + w0, n1 + e0, s0 + w1, s1 + e1
        z = jnp.where(
            lane == 0, nw, jnp.where(lane == 1, ne, jnp.where(lane == 2, sw, se))
        )
        first = z[0:LANES].T[0:4]
        if z.shape[0] > s2:
            spare = jnp.zeros((2 * LANES - z.shape[0], LANES), jnp.float32)
            second = jnp.concatenate([z[LANES:], spare], axis=0).T[0:4]
        else:
            second = jnp.zeros_like(first)
        corner_out[e % 2] = jnp.concatenate([first, second], axis=0)
        for k in range(4):
            corner_copy(e, k).start()

    chunk = part.shape[2]

    def stage_a(a, j):
        d = j
        target = lax.rem(sy + d, nsy)
        return pltpu.make_async_remote_copy(
            src_ref=part.at[a, target // nx],
            dst_ref=plane_in.at[a, nsy - d],
            send_sem=asend_sem.at[a, 0],
            recv_sem=arecv_sem.at[a, 0],
            device_id=dev(target, sx),
            device_id_type=MESH,
        )

    def stage_b(a, d):
        return pltpu.make_async_remote_copy(
            src_ref=line_out.at[a],
            dst_ref=line_in.at[a, nz - d],
            send_sem=asend_sem.at[a, 1],
            recv_sem=arecv_sem.at[a, 1],
            device_id=dev(sy, lax.rem(sx + d, nz)),
            device_id_type=MESH,
        )

    def stage_c(a, d):
        return pltpu.make_async_remote_copy(
            src_ref=col_out.at[a],
            dst_ref=col_in.at[a, ny - d],
            send_sem=asend_sem.at[a, 2],
            recv_sem=arecv_sem.at[a, 2],
            device_id=dev(lax.rem(sy + d * nx, nsy), sx),
            device_id_type=MESH,
        )

    def whole(a, stage):
        buf = (plane_in, line_in, col_in)[stage]
        n = (nsy, nz, ny)[stage]
        ref = buf.at[a, pl.ds(1, n - 1)]
        return pltpu.make_async_remote_copy(
            src_ref=ref,
            dst_ref=ref,
            send_sem=asend_sem.at[a, stage],
            recv_sem=arecv_sem.at[a, stage],
            device_id=peer[EAST],
            device_id_type=MESH,
        )

    def summed(values):
        while len(values) > 1:
            values = [
                values[i] + values[i + 1] if i + 1 < len(values) else values[i]
                for i in range(0, len(values), 2)
            ]
        return values[0]

    def start_sum(a, payload):
        for j in range(ny):
            part[a, j] = payload[j * chunk : (j + 1) * chunk]
        for d in range(1, nsy):
            stage_a(a, d).start()

    def sum_b(a):
        whole(a, 0).wait_recv()
        plane_in[a, 0] = part[a, yy]
        line_out[a] = summed([plane_in[a, lax.rem(j - sy + nsy, nsy)] for j in range(nsy)])
        for d in range(1, nz):
            stage_b(a, d).start()

    def sum_c(a):
        whole(a, 1).wait_recv()
        line_in[a, 0] = line_out[a]
        col_out[a] = summed([line_in[a, lax.rem(j - sx + nz, nz)] for j in range(nz)])
        for d in range(1, ny):
            stage_c(a, d).start()

    def sum_end(a):
        whole(a, 2).wait_recv()
        col_in[a, 0] = col_out[a]
        return jnp.concatenate([col_in[a, lax.rem(j - yy + ny, ny)] for j in range(ny)], axis=0)

    for t in order:
        for side in range(4):
            side_copy(1, side, t).start()
    send_corners(1, lambda side, t: src_ref[side, t])

    res = res_ref[...]
    res_hi = res.astype(jnp.bfloat16)
    res_split[0:q2] = res_hi
    res_split[q2:] = (res - res_hi.astype(jnp.float32)).astype(jnp.bfloat16)
    lhs[s2:rows_all] = pro_ref[...].astype(jnp.bfloat16)

    def restrict(first, last):
        hi, lo = lhs[first:last], low[first:last]
        half = (last - first) // 2
        both = dot(res_split[...], hi, ((1,), (1,)))
        rest = dot(res_split[0:q2], lo, ((1,), (1,)))
        u = both[0:q2] + both[q2:] + rest
        return u[0:half_q] + turned(u[half_q:], half)

    def coarse(total):
        stacked = jnp.concatenate([total, turned(total, half_s)], axis=0)
        coef = dot(inv_ref[...], stacked, ((0,), (0,)), HIGH)
        return coef

    def stack_of(coef):
        return jnp.concatenate([coef, turned(coef, half_s)], axis=0)

    def lifted(coef, k):
        fix[...] = dot(stack_of(coef), lift[k], ((0,), (0,)), HIGH)

    def receive(e, fixed):
        par, rows = e % 2, rows_of(e)
        for k in range(4):
            corner_copy(e, k).wait_recv()
        tile = []
        for base in (0, 4) if rows > s2 else (0,):
            for k in range(4):
                row = corner_in[par, k, base + 3 - k : base + 4 - k]
                tile.append(jnp.where(has_diag[k], 0.5 * row, 0.0))
        spare = jnp.zeros((LANES - len(tile), LANES), jnp.float32)
        flat = jnp.concatenate([*tile, spare], axis=0).T
        cols = flat[:, 0:4]
        if rows > s2:
            cols = jnp.concatenate([cols, flat[0:q2, 4:8]], axis=0)
        nw, ne, sw, se = (cols[:, k : k + 1] for k in range(4))
        ends = {NORTH: (nw, ne), SOUTH: (sw, se), WEST: (nw, sw), EAST: (ne, se)}

        def incoming(side, t, first, last):
            value = jnp.where(has[side], got[par, side, t, first:last], 0.0)
            if t == 0:
                value += jnp.where(lane == 0, ends[side][0][first:last], 0.0)
            if t == thirds - 1:
                value += jnp.where(lane == LANES - 1, ends[side][1][first:last], 0.0)
            return value

        for t in order:
            for side in range(4):
                side_copy(e, OUT_OF[side], t).wait_recv()
                if rows > s2:
                    at = side * cells + t * LANES
                    extra = incoming(side, t, s2, rows)
                    hi = extra.astype(jnp.bfloat16)
                    lift[e - 2, :, at : at + LANES] = extra
                    lhs[s2:, at : at + LANES] = hi
                    low[s2:, at : at + LANES] = (extra - hi.astype(jnp.float32)).astype(jnp.bfloat16)
        if fixed is not None:
            lifted(fixed, 1)
        for t in order:
            for side in range(4):
                at = side * cells + t * LANES
                top = incoming(side, t, 0, s2)
                if fixed is not None:
                    top += fix[:, at : at + LANES]
                if e == ITERS:
                    out_ref[:, at : at + LANES] = top
                    continue
                hi = top.astype(jnp.bfloat16)
                lhs[0:s2, at : at + LANES] = hi
                low[0:s2, at : at + LANES] = (top - hi.astype(jnp.float32)).astype(jnp.bfloat16)
        for t in order:
            for side in range(4):
                side_copy(e, side, t).wait_send()
        for k in range(4):
            corner_copy(e, k).wait_send()

    def multiply(e):
        rows = rows_of(e)

        for t in (*order, None):
            if t == order[-1]:
                send_corners(e, lambda side, t: sent[side, t, 0:rows])
            if t is None:
                break
            for h in (0, 1):
                if e == 2:
                    loads[t][h].wait()
                product = dot(lhs[0:rows], table[t, h], ((1,), (0,)))
                for k in (0, 1):
                    side = 2 * h + k
                    re = product[:, 2 * k * LANES : (2 * k + 1) * LANES]
                    im = product[:, (2 * k + 1) * LANES : (2 * k + 2) * LANES]
                    a, b = half_s, s2
                    sent[side, t, 0:a] = re[0:a] - im[a:b] + src_ref[side, t, 0:a]
                    sent[side, t, a:b] = im[0:a] + re[a:b] + src_ref[side, t, a:b]
                    if rows > s2:
                        a, b = s2 + half_q, s2 + q2
                        sent[side, t, s2:a] = re[s2:a] - im[a:b]
                        sent[side, t, a:b] = im[s2:a] + re[a:b]
                    side_copy(e, side, t).start()

    coef = {}
    for i in range(1, ITERS + 1):
        if i == 3:
            sum_c(1)
            coef[1] = coarse(sum_end(1))
        elif i > 3:
            finish(i - 2)
        receive(i, coef.get(i - 2))
        if i == ITERS:
            break
        start_sum(i, restrict(0, s2))
        if i == 2:
            half = restrict(s2, rows_all)
            start_sum(0, jnp.concatenate([half, jnp.zeros((half_q, LANES - q2), jnp.float32)], axis=1))
        multiply(i + 1)
        sum_b(i)
        if i == 2:
            sum_b(0)
            sum_c(0)
            share = sum_end(0)[:, 0:q2]

            def finish(j):
                sum_c(j)
                total = sum_end(j) + dot(share, stack_of(coef[j - 1]), ((1,), (0,)), HIGH)
                coef[j] = coarse(total)

    finish(ITERS - 1)
    lifted(coef[ITERS - 1], 0)
    for side in range(4):
        for t in range(thirds):
            at = side * cells + t * LANES
            out_ref[:, at : at + LANES] += fix[:, at : at + LANES]
    coef_ref[...] = coef[ITERS - 1]
    for a in range(ITERS):
        for stage in range(3):
            whole(a, stage).wait_send()


def solution(mesh):
    nsy, nz = mesh.shape["sy"], mesh.shape["sx"]
    nx = 4
    ny = nsy // nx

    def per_device(interface_map, source_trace, restriction, prolongation, coarse_inverse):
        src_count, cells = source_trace.shape[3], source_trace.shape[5]
        width = restriction.shape[3]
        thirds = cells // LANES
        s2, q2 = 2 * src_count, 2 * width
        rows = s2 + q2
        depth = 4 * cells
        dims = (ny, nx, nz, s2, q2, thirds)
        table = interface_map.reshape(depth, 2, 2, 2, thirds, LANES)
        table = table.transpose(4, 2, 0, 3, 1, 5).reshape(thirds, 2, depth, 4 * LANES)
        sources = source_trace.reshape(s2, 4, thirds, LANES).transpose(1, 2, 0, 3)
        chunk = width // ny
        vmem = pl.BlockSpec(memory_space=pltpu.VMEM)
        traces, coef = pl.pallas_call(
            functools.partial(kernel, dims),
            out_shape=(
                jax.ShapeDtypeStruct((s2, depth), jnp.float32),
                jax.ShapeDtypeStruct((width, s2), jnp.float32),
            ),
            in_specs=[pl.BlockSpec(memory_space=pl.ANY), vmem, vmem, vmem, vmem],
            out_specs=(vmem, vmem),
            scratch_shapes=[
                pltpu.VMEM((thirds, 2, depth, 4 * LANES), jnp.bfloat16),
                pltpu.VMEM((rows, depth), jnp.bfloat16),
                pltpu.VMEM((rows, depth), jnp.bfloat16),
                pltpu.VMEM((4, thirds, rows, LANES), jnp.float32),
                pltpu.VMEM((2, 4, thirds, rows, LANES), jnp.float32),
                pltpu.VMEM((2, q2, depth), jnp.float32),
                pltpu.VMEM((2 * q2, depth), jnp.bfloat16),
                pltpu.VMEM((2, 8, LANES), jnp.float32),
                pltpu.VMEM((2, 4, 8, LANES), jnp.float32),
                pltpu.VMEM((ITERS, ny, chunk, LANES), jnp.float32),
                pltpu.VMEM((ITERS, nsy, chunk, LANES), jnp.float32),
                pltpu.VMEM((ITERS, chunk, LANES), jnp.float32),
                pltpu.VMEM((ITERS, nz, chunk, LANES), jnp.float32),
                pltpu.VMEM((ITERS, chunk, LANES), jnp.float32),
                pltpu.VMEM((ITERS, ny, chunk, LANES), jnp.float32),
                pltpu.VMEM((s2, depth), jnp.float32),
                pltpu.SemaphoreType.DMA((thirds, 2)),
                pltpu.SemaphoreType.DMA((4, thirds)),
                pltpu.SemaphoreType.DMA((2, 4, thirds)),
                pltpu.SemaphoreType.DMA((2, 4)),
                pltpu.SemaphoreType.DMA((2, 4)),
                pltpu.SemaphoreType.DMA((ITERS, 3)),
                pltpu.SemaphoreType.DMA((ITERS, 3)),
            ],
            compiler_params=pltpu.CompilerParams(
                collective_id=0, has_side_effects=True, vmem_limit_bytes=60 * 1024 * 1024
            ),
        )(
            table,
            sources,
            restriction.reshape(q2, depth),
            prolongation.reshape(q2, depth),
            coarse_inverse.reshape(q2, width),
        )
        coef = coef.reshape(width, 2, src_count).transpose(1, 2, 0)
        return traces.reshape(source_trace.shape), coef

    where = P(("wl", "sy"), "sx", None, None, None, None)
    return jax.shard_map(
        per_device,
        mesh=mesh,
        in_specs=(P(("wl", "sy"), "sx", None, None, None), where, where, where, P("wl", None, None)),
        out_specs=(where, P("wl", None, None)),
        check_vma=False,
    )
```

```python
import functools

import jax
import jax.numpy as jnp
from jax import lax
from jax.experimental import pallas as pl
from jax.experimental.pallas import tpu as pltpu
from jax.sharding import PartitionSpec as P

ITERS = 6
LANES = 128
MESH = pl.DeviceIdType.MESH
HIGH = lax.Precision.HIGHEST
NORTH, SOUTH, WEST, EAST = 0, 1, 2, 3
OUT_OF = {NORTH: SOUTH, SOUTH: NORTH, WEST: EAST, EAST: WEST}


def dot(a, b, contract, precision=None):
    return lax.dot_general(
        a, b, (contract, ((), ())), preferred_element_type=jnp.float32, precision=precision
    )


def turned(pair, half):
    return jnp.concatenate([-pair[:, half:], pair[:, :half]], axis=1)


def kernel(
    dims,
    map_hbm,
    src_hbm,
    res_hbm,
    pro_hbm,
    inv_ref,
    out_hbm,
    coef_ref,
    raw,
    src_raw,
    res_raw,
    pro_raw,
    src_ref,
    table,
    lhs,
    low,
    sent,
    got,
    lift,
    res_split,
    corner_out,
    corner_in,
    part,
    plane_in,
    line_out,
    line_in,
    col_out,
    col_in,
    fix,
    last_sum,
    map_sem,
    load_sem,
    send_sem,
    recv_sem,
    csend_sem,
    crecv_sem,
    asend_sem,
    arecv_sem,
):
    ny, nx, nz, s2, q2, thirds = dims
    cells = thirds * LANES
    nsy = ny * nx
    rows_all = s2 + q2
    half_s, half_q = s2 // 2, q2 // 2
    sy, sx = lax.axis_index("sy"), lax.axis_index("sx")
    wl = lax.axis_index("wl")
    yy = sy // nx

    def dev(row, col):
        return (row, col, wl)

    up, down = lax.rem(sy + nsy - 1, nsy), lax.rem(sy + 1, nsy)
    left, right = lax.rem(sx + nz - 1, nz), lax.rem(sx + 1, nz)
    peer = {NORTH: dev(up, sx), SOUTH: dev(down, sx), WEST: dev(sy, left), EAST: dev(sy, right)}
    diag = (dev(up, left), dev(up, right), dev(down, left), dev(down, right))
    has = {NORTH: sy > 0, SOUTH: sy < nsy - 1, WEST: sx > 0, EAST: sx < nz - 1}
    has_diag = (
        (sy > 0) & (sx > 0),
        (sy > 0) & (sx < nz - 1),
        (sy < nsy - 1) & (sx > 0),
        (sy < nsy - 1) & (sx < nz - 1),
    )

    depth = 4 * cells
    order = (0, *range(2, thirds), 1)
    blocks = depth // LANES
    flat_map = map_hbm.reshape(2 * depth, depth)
    loads = [
        pltpu.make_async_copy(
            flat_map.at[pl.ds(2 * LANES * b, 2 * LANES)],
            raw.at[pl.ds(2 * LANES * b, 2 * LANES)],
            map_sem.at[b],
        )
        for b in range(blocks)
    ]
    flat_src = src_hbm.reshape(4 * s2, cells)
    flat_pro = pro_hbm.reshape(4 * q2, cells)
    flat_res = res_hbm.reshape(4 * q2, cells)

    def third(flat, held, which):
        return [
            pltpu.make_async_copy(
                flat.at[:, pl.ds(t * LANES, LANES)], held.at[t], load_sem.at[which, t]
            )
            for t in range(thirds)
        ]

    src_load = third(flat_src, src_raw, 0)
    pro_load = third(flat_pro, pro_raw, 1)
    res_load = third(flat_res, res_raw, 2)
    for copy in (*src_load, *pro_load, *res_load):
        copy.start()
    for b in range(blocks):
        loads[b].start()

    barrier = pltpu.get_barrier_semaphore()
    met = 0
    for target in (*peer.values(), *diag):
        pl.semaphore_signal(barrier, inc=1, device_id=target, device_id_type=MESH)
        met += 1
    for d in range(1, nsy):
        target = dev(lax.rem(sy + d, nsy), sx)
        pl.semaphore_signal(barrier, inc=1, device_id=target, device_id_type=MESH)
        met += 1
    for d in range(1, nz):
        target = dev(sy, lax.rem(sx + d, nz))
        pl.semaphore_signal(barrier, inc=1, device_id=target, device_id_type=MESH)
        met += 1
    for t in order:
        src_load[t].wait()
        for side in range(4):
            src_ref[side, t] = src_raw[t, pl.ds(side, s2, stride=4), :]
    pl.semaphore_wait(barrier, met)

    lane = lax.broadcasted_iota(jnp.int32, (1, LANES), 1)

    def rows_of(e):
        return rows_all if e in (2, 3) else s2

    def side_copy(e, side, t):
        par, rows = e % 2, rows_of(e)
        src = src_ref.at[side, t] if e == 1 else sent.at[side, t, pl.ds(0, rows)]
        return pltpu.make_async_remote_copy(
            src_ref=src,
            dst_ref=got.at[par, OUT_OF[side], t, pl.ds(0, rows)],
            send_sem=send_sem.at[side, t],
            recv_sem=recv_sem.at[par, OUT_OF[side], t],
            device_id=peer[side],
            device_id_type=MESH,
        )

    def corner_copy(e, k):
        par = e % 2
        return pltpu.make_async_remote_copy(
            src_ref=corner_out.at[par],
            dst_ref=corner_in.at[par, 3 - k],
            send_sem=csend_sem.at[par, k],
            recv_sem=crecv_sem.at[par, 3 - k],
            device_id=diag[k],
            device_id_type=MESH,
        )

    def send_corners(e, block):
        last = thirds - 1
        n0, n1 = block(NORTH, 0)[:, 0:1], block(NORTH, last)[:, LANES - 1 :]
        s0, s1 = block(SOUTH, 0)[:, 0:1], block(SOUTH, last)[:, LANES - 1 :]
        w0, w1 = block(WEST, 0)[:, 0:1], block(WEST, last)[:, LANES - 1 :]
        e0, e1 = block(EAST, 0)[:, 0:1], block(EAST, last)[:, LANES - 1 :]
        nw, ne, sw, se = n0 + w0, n1 + e0, s0 + w1, s1 + e1
        z = jnp.where(
            lane == 0, nw, jnp.where(lane == 1, ne, jnp.where(lane == 2, sw, se))
        )
        first = z[0:LANES].T[0:4]
        if z.shape[0] > s2:
            spare = jnp.zeros((2 * LANES - z.shape[0], LANES), jnp.float32)
            second = jnp.concatenate([z[LANES:], spare], axis=0).T[0:4]
        else:
            second = jnp.zeros_like(first)
        corner_out[e % 2] = jnp.concatenate([first, second], axis=0)
        for k in range(4):
            corner_copy(e, k).start()

    chunk = part.shape[2]

    def stage_a(a, j):
        d = j
        target = lax.rem(sy + d, nsy)
        return pltpu.make_async_remote_copy(
            src_ref=part.at[a, target // nx],
            dst_ref=plane_in.at[a, nsy - d],
            send_sem=asend_sem.at[a, 0],
            recv_sem=arecv_sem.at[a, 0],
            device_id=dev(target, sx),
            device_id_type=MESH,
        )

    def stage_b(a, d):
        return pltpu.make_async_remote_copy(
            src_ref=line_out.at[a],
            dst_ref=line_in.at[a, nz - d],
            send_sem=asend_sem.at[a, 1],
            recv_sem=arecv_sem.at[a, 1],
            device_id=dev(sy, lax.rem(sx + d, nz)),
            device_id_type=MESH,
        )

    def stage_c(a, d):
        return pltpu.make_async_remote_copy(
            src_ref=col_out.at[a],
            dst_ref=col_in.at[a, ny - d],
            send_sem=asend_sem.at[a, 2],
            recv_sem=arecv_sem.at[a, 2],
            device_id=dev(lax.rem(sy + d * nx, nsy), sx),
            device_id_type=MESH,
        )

    def whole(a, stage):
        buf = (plane_in, line_in, col_in)[stage]
        n = (nsy, nz, ny)[stage]
        ref = buf.at[a, pl.ds(1, n - 1)]
        return pltpu.make_async_remote_copy(
            src_ref=ref,
            dst_ref=ref,
            send_sem=asend_sem.at[a, stage],
            recv_sem=arecv_sem.at[a, stage],
            device_id=peer[EAST],
            device_id_type=MESH,
        )

    def summed(values):
        while len(values) > 1:
            values = [
                values[i] + values[i + 1] if i + 1 < len(values) else values[i]
                for i in range(0, len(values), 2)
            ]
        return values[0]

    def start_sum(a, payload):
        for j in range(ny):
            part[a, j] = payload[j * chunk : (j + 1) * chunk]
        for d in range(1, nsy):
            stage_a(a, d).start()

    def sum_b(a):
        whole(a, 0).wait_recv()
        plane_in[a, 0] = part[a, yy]
        line_out[a] = summed([plane_in[a, lax.rem(j - sy + nsy, nsy)] for j in range(nsy)])
        for d in range(1, nz):
            stage_b(a, d).start()

    def sum_c(a):
        whole(a, 1).wait_recv()
        line_in[a, 0] = line_out[a]
        col_out[a] = summed([line_in[a, lax.rem(j - sx + nz, nz)] for j in range(nz)])
        for d in range(1, ny):
            stage_c(a, d).start()

    def sum_end(a):
        whole(a, 2).wait_recv()
        col_in[a, 0] = col_out[a]
        return jnp.concatenate([col_in[a, lax.rem(j - yy + ny, ny)] for j in range(ny)], axis=0)

    for t in order:
        for side in range(4):
            side_copy(1, side, t).start()
    send_corners(1, lambda side, t: src_ref[side, t])

    for t in order:
        pro_load[t].wait()
        res_load[t].wait()
        for side in range(4):
            at = side * cells + t * LANES
            lhs[s2:rows_all, at : at + LANES] = pro_raw[t, pl.ds(side, q2, stride=4), :].astype(
                jnp.bfloat16
            )
            res = res_raw[t, pl.ds(side, q2, stride=4), :]
            res_hi = res.astype(jnp.bfloat16)
            res_split[0:q2, at : at + LANES] = res_hi
            res_split[q2:, at : at + LANES] = (res - res_hi.astype(jnp.float32)).astype(jnp.bfloat16)

    rows_i = lax.broadcasted_iota(jnp.int32, (2 * LANES, 2 * LANES), 0)
    cols_i = lax.broadcasted_iota(jnp.int32, (2 * LANES, 2 * LANES), 1)
    wanted = jnp.where(rows_i < LANES, 2 * rows_i, 2 * (rows_i - LANES) + 1)
    chosen = jnp.where(cols_i == wanted, 1.0, 0.0).astype(jnp.bfloat16)
    for b in range(blocks):
        loads[b].wait()
        parted = dot(chosen, raw[2 * LANES * b : 2 * LANES * (b + 1)], ((1,), (0,)))
        parted = parted.astype(jnp.bfloat16)
        for side in range(4):
            h, k = side // 2, 2 * (side % 2) * LANES
            for t in range(thirds):
                at = side * cells + t * LANES
                for c in (0, 1):
                    table[t, h, b * LANES : (b + 1) * LANES, k + c * LANES : k + (c + 1) * LANES] = parted[
                        c * LANES : (c + 1) * LANES, at : at + LANES
                    ]

    def restrict(first, last):
        hi, lo = lhs[first:last], low[first:last]
        half = (last - first) // 2
        both = dot(res_split[...], hi, ((1,), (1,)))
        rest = dot(res_split[0:q2], lo, ((1,), (1,)))
        u = both[0:q2] + both[q2:] + rest
        return u[0:half_q] + turned(u[half_q:], half)

    def coarse(total):
        stacked = jnp.concatenate([total, turned(total, half_s)], axis=0)
        coef = dot(inv_ref[...], stacked, ((0,), (0,)), HIGH)
        return coef

    def stack_of(coef):
        return jnp.concatenate([coef, turned(coef, half_s)], axis=0)

    def lifted(coef, k):
        fix[...] = dot(stack_of(coef), lift[k], ((0,), (0,)), HIGH)

    def receive(e, fixed):
        par, rows = e % 2, rows_of(e)
        for k in range(4):
            corner_copy(e, k).wait_recv()
        tile = []
        for base in (0, 4) if rows > s2 else (0,):
            for k in range(4):
                row = corner_in[par, k, base + 3 - k : base + 4 - k]
                tile.append(jnp.where(has_diag[k], 0.5 * row, 0.0))
        spare = jnp.zeros((LANES - len(tile), LANES), jnp.float32)
        flat = jnp.concatenate([*tile, spare], axis=0).T
        cols = flat[:, 0:4]
        if rows > s2:
            cols = jnp.concatenate([cols, flat[0:q2, 4:8]], axis=0)
        nw, ne, sw, se = (cols[:, k : k + 1] for k in range(4))
        ends = {NORTH: (nw, ne), SOUTH: (sw, se), WEST: (nw, sw), EAST: (ne, se)}

        def incoming(side, t, first, last):
            value = jnp.where(has[side], got[par, side, t, first:last], 0.0)
            if t == 0:
                value += jnp.where(lane == 0, ends[side][0][first:last], 0.0)
            if t == thirds - 1:
                value += jnp.where(lane == LANES - 1, ends[side][1][first:last], 0.0)
            return value

        if fixed is not None and rows == s2:
            lifted(fixed, 1)
        for t in order:
            for side in range(4):
                side_copy(e, OUT_OF[side], t).wait_recv()
                if rows > s2:
                    at = side * cells + t * LANES
                    extra = incoming(side, t, s2, rows)
                    hi = extra.astype(jnp.bfloat16)
                    lift[e - 2, :, at : at + LANES] = extra
                    lhs[s2:, at : at + LANES] = hi
                    low[s2:, at : at + LANES] = (extra - hi.astype(jnp.float32)).astype(jnp.bfloat16)
        if fixed is not None and rows > s2:
            lifted(fixed, 1)
        for t in order:
            for side in range(4):
                at = side * cells + t * LANES
                top = incoming(side, t, 0, s2)
                if fixed is not None:
                    top += fix[:, at : at + LANES]
                if e == ITERS:
                    last_sum[:, at : at + LANES] = top
                    continue
                hi = top.astype(jnp.bfloat16)
                lhs[0:s2, at : at + LANES] = hi
                low[0:s2, at : at + LANES] = (top - hi.astype(jnp.float32)).astype(jnp.bfloat16)
        for t in order:
            for side in range(4):
                side_copy(e, side, t).wait_send()
        for k in range(4):
            corner_copy(e, k).wait_send()

    def multiply(e):
        rows = rows_of(e)

        for t in (*order, None):
            if t == order[-1]:
                send_corners(e, lambda side, t: sent[side, t, 0:rows])
            if t is None:
                break
            for h in (0, 1):
                product = dot(lhs[0:rows], table[t, h], ((1,), (0,)))
                for k in (0, 1):
                    side = 2 * h + k
                    re = product[:, 2 * k * LANES : (2 * k + 1) * LANES]
                    im = product[:, (2 * k + 1) * LANES : (2 * k + 2) * LANES]
                    a, b = half_s, s2
                    sent[side, t, 0:a] = re[0:a] - im[a:b] + src_ref[side, t, 0:a]
                    sent[side, t, a:b] = im[0:a] + re[a:b] + src_ref[side, t, a:b]
                    if rows > s2:
                        a, b = s2 + half_q, s2 + q2
                        sent[side, t, s2:a] = re[s2:a] - im[a:b]
                        sent[side, t, a:b] = im[s2:a] + re[a:b]
                    side_copy(e, side, t).start()

    coef = {}
    share = None
    for i in range(1, ITERS + 1):
        if i == 3:
            coef[1] = coarse(sum_end(1))
        elif i > 3:
            if i == 4:
                share = sum_end(0)[:, 0:q2]
            total = sum_end(i - 2) + dot(share, stack_of(coef[i - 3]), ((1,), (0,)), HIGH)
            coef[i - 2] = coarse(total)
        receive(i, coef.get(i - 2))
        if i == ITERS:
            break
        start_sum(i, restrict(0, s2))
        if i == 2:
            half = restrict(s2, rows_all)
            start_sum(0, jnp.concatenate([half, jnp.zeros((half_q, LANES - q2), jnp.float32)], axis=1))
        multiply(i + 1)
        if i >= 2:
            sum_c(i - 1)
        if i == 3:
            sum_c(0)
        sum_b(i)
        if i == 2:
            sum_b(0)
        if i == ITERS - 1:
            sum_c(i)

    total = sum_end(ITERS - 1) + dot(share, stack_of(coef[ITERS - 2]), ((1,), (0,)), HIGH)
    coef[ITERS - 1] = coarse(total)
    lifted(coef[ITERS - 1], 0)
    flat_out = out_hbm.reshape(4 * s2, cells)
    stores = [
        pltpu.make_async_copy(
            src_raw.at[t], flat_out.at[:, pl.ds(t * LANES, LANES)], load_sem.at[0, t]
        )
        for t in range(thirds)
    ]
    for t in range(thirds):
        for side in range(4):
            at = side * cells + t * LANES
            src_raw[t, pl.ds(side, s2, stride=4), :] = (
                last_sum[:, at : at + LANES] + fix[:, at : at + LANES]
            )
        stores[t].start()
    spare = jnp.zeros((LANES - half_q, s2), jnp.float32)
    coef_ref[...] = jnp.concatenate([coef[ITERS - 1], spare], axis=0).T[:, 0:half_q]
    for a in range(ITERS):
        for stage in range(3):
            whole(a, stage).wait_send()
    for t in range(thirds):
        stores[t].wait()


def solution(mesh):
    nsy, nz = mesh.shape["sy"], mesh.shape["sx"]
    nx = 4
    ny = nsy // nx

    def per_device(interface_map, source_trace, restriction, prolongation, coarse_inverse):
        src_count, cells = source_trace.shape[3], source_trace.shape[5]
        width = restriction.shape[3]
        thirds = cells // LANES
        s2, q2 = 2 * src_count, 2 * width
        rows = s2 + q2
        depth = 4 * cells
        dims = (ny, nx, nz, s2, q2, thirds)
        chunk = width // ny
        vmem = pl.BlockSpec(memory_space=pltpu.VMEM)
        hbm = pl.BlockSpec(memory_space=pl.ANY)
        traces, coef = pl.pallas_call(
            functools.partial(kernel, dims),
            out_shape=(
                jax.ShapeDtypeStruct((2, src_count, 4, cells), jnp.float32),
                jax.ShapeDtypeStruct((s2, width), jnp.float32),
            ),
            in_specs=[hbm, hbm, hbm, hbm, vmem],
            out_specs=(hbm, vmem),
            scratch_shapes=[
                pltpu.VMEM((2 * depth, depth), jnp.bfloat16),
                pltpu.VMEM((thirds, 4 * s2, LANES), jnp.float32),
                pltpu.VMEM((thirds, 4 * q2, LANES), jnp.float32),
                pltpu.VMEM((thirds, 4 * q2, LANES), jnp.float32),
                pltpu.VMEM((4, thirds, s2, LANES), jnp.float32),
                pltpu.VMEM((thirds, 2, depth, 4 * LANES), jnp.bfloat16),
                pltpu.VMEM((rows, depth), jnp.bfloat16),
                pltpu.VMEM((rows, depth), jnp.bfloat16),
                pltpu.VMEM((4, thirds, rows, LANES), jnp.float32),
                pltpu.VMEM((2, 4, thirds, rows, LANES), jnp.float32),
                pltpu.VMEM((2, q2, depth), jnp.float32),
                pltpu.VMEM((2 * q2, depth), jnp.bfloat16),
                pltpu.VMEM((2, 8, LANES), jnp.float32),
                pltpu.VMEM((2, 4, 8, LANES), jnp.float32),
                pltpu.VMEM((ITERS, ny, chunk, LANES), jnp.float32),
                pltpu.VMEM((ITERS, nsy, chunk, LANES), jnp.float32),
                pltpu.VMEM((ITERS, chunk, LANES), jnp.float32),
                pltpu.VMEM((ITERS, nz, chunk, LANES), jnp.float32),
                pltpu.VMEM((ITERS, chunk, LANES), jnp.float32),
                pltpu.VMEM((ITERS, ny, chunk, LANES), jnp.float32),
                pltpu.VMEM((s2, depth), jnp.float32),
                pltpu.VMEM((s2, depth), jnp.float32),
                pltpu.SemaphoreType.DMA((depth // LANES,)),
                pltpu.SemaphoreType.DMA((3, thirds)),
                pltpu.SemaphoreType.DMA((4, thirds)),
                pltpu.SemaphoreType.DMA((2, 4, thirds)),
                pltpu.SemaphoreType.DMA((2, 4)),
                pltpu.SemaphoreType.DMA((2, 4)),
                pltpu.SemaphoreType.DMA((ITERS, 3)),
                pltpu.SemaphoreType.DMA((ITERS, 3)),
            ],
            compiler_params=pltpu.CompilerParams(
                collective_id=0, has_side_effects=True, vmem_limit_bytes=60 * 1024 * 1024
            ),
        )(
            interface_map.reshape(depth, 2, depth),
            source_trace.reshape(2, src_count, 4, cells),
            restriction.reshape(2, width, 4, cells),
            prolongation.reshape(2, width, 4, cells),
            coarse_inverse.reshape(q2, width),
        )
        return traces.reshape(source_trace.shape), coef.reshape(2, src_count, width)

    where = P(("wl", "sy"), "sx", None, None, None, None)
    return jax.shard_map(
        per_device,
        mesh=mesh,
        in_specs=(P(("wl", "sy"), "sx", None, None, None), where, where, where, P("wl", None, None)),
        out_specs=(where, P("wl", None, None)),
        check_vma=False,
    )
```

```python
import functools

import jax
import jax.numpy as jnp
from jax import lax
from jax.experimental import pallas as pl
from jax.experimental.pallas import tpu as pltpu
from jax.sharding import PartitionSpec as P

ITERS = 6
LANES = 128
MESH = pl.DeviceIdType.MESH
HIGH = lax.Precision.HIGHEST
NORTH, SOUTH, WEST, EAST = 0, 1, 2, 3
OUT_OF = {NORTH: SOUTH, SOUTH: NORTH, WEST: EAST, EAST: WEST}


def dot(a, b, contract, precision=None):
    return lax.dot_general(
        a, b, (contract, ((), ())), preferred_element_type=jnp.float32, precision=precision
    )


def turned(pair, half):
    return jnp.concatenate([-pair[:, half:], pair[:, :half]], axis=1)


def kernel(
    dims,
    map_hbm,
    src_hbm,
    res_hbm,
    pro_hbm,
    inv_ref,
    out_hbm,
    coef_ref,
    raw,
    src_raw,
    res_raw,
    pro_raw,
    src_ref,
    table,
    lhs,
    acc,
    out_hi,
    out_lo,
    sent,
    got,
    lift,
    res_split,
    corner_out,
    corner_in,
    part,
    plane_in,
    line_out,
    line_in,
    col_out,
    col_in,
    fix,
    last_sum,
    map_sem,
    load_sem,
    send_sem,
    recv_sem,
    csend_sem,
    crecv_sem,
    asend_sem,
    arecv_sem,
):
    ny, nx, nz, s2, q2, thirds = dims
    cells = thirds * LANES
    nsy = ny * nx
    rows_all = s2 + q2
    half_s, half_q = s2 // 2, q2 // 2
    sy, sx = lax.axis_index("sy"), lax.axis_index("sx")
    wl = lax.axis_index("wl")
    yy = sy // nx

    def dev(row, col):
        return (row, col, wl)

    def place(side, t):
        return (order.index(t) * 4 + side) * LANES

    up, down = lax.rem(sy + nsy - 1, nsy), lax.rem(sy + 1, nsy)
    left, right = lax.rem(sx + nz - 1, nz), lax.rem(sx + 1, nz)
    peer = {NORTH: dev(up, sx), SOUTH: dev(down, sx), WEST: dev(sy, left), EAST: dev(sy, right)}
    diag = (dev(up, left), dev(up, right), dev(down, left), dev(down, right))
    has = {NORTH: sy > 0, SOUTH: sy < nsy - 1, WEST: sx > 0, EAST: sx < nz - 1}
    has_diag = (
        (sy > 0) & (sx > 0),
        (sy > 0) & (sx < nz - 1),
        (sy < nsy - 1) & (sx > 0),
        (sy < nsy - 1) & (sx < nz - 1),
    )

    depth = 4 * cells
    order = (0, *range(2, thirds), 1)
    early = 4 * LANES * (thirds - 1)
    blocks = depth // LANES
    flat_map = map_hbm.reshape(2 * depth, depth)
    loads = [
        pltpu.make_async_copy(
            flat_map.at[pl.ds(2 * LANES * b, 2 * LANES)],
            raw.at[pl.ds(2 * LANES * b, 2 * LANES)],
            map_sem.at[b],
        )
        for b in range(blocks)
    ]
    flat_src = src_hbm.reshape(4 * s2, cells)
    flat_pro = pro_hbm.reshape(4 * q2, cells)
    flat_res = res_hbm.reshape(4 * q2, cells)

    def third(flat, held, which):
        return [
            pltpu.make_async_copy(
                flat.at[:, pl.ds(t * LANES, LANES)], held.at[t], load_sem.at[which, t]
            )
            for t in range(thirds)
        ]

    src_load = third(flat_src, src_raw, 0)
    pro_load = third(flat_pro, pro_raw, 1)
    res_load = third(flat_res, res_raw, 2)
    for copy in (*src_load, *pro_load, *res_load):
        copy.start()
    for b in range(blocks):
        loads[b].start()

    barrier = pltpu.get_barrier_semaphore()
    met = 0
    for target in (*peer.values(), *diag):
        pl.semaphore_signal(barrier, inc=1, device_id=target, device_id_type=MESH)
        met += 1
    for d in range(1, nsy):
        target = dev(lax.rem(sy + d, nsy), sx)
        pl.semaphore_signal(barrier, inc=1, device_id=target, device_id_type=MESH)
        met += 1
    for d in range(1, nz):
        target = dev(sy, lax.rem(sx + d, nz))
        pl.semaphore_signal(barrier, inc=1, device_id=target, device_id_type=MESH)
        met += 1
    for t in order:
        src_load[t].wait()
        res_load[t].wait()
        for side in range(4):
            at = place(side, t)
            value = src_raw[t, pl.ds(side, s2, stride=4), :]
            src_ref[side, t] = value
            sent[1, side, t, 0:s2] = value
            sent[1, side, t, s2:] = res_raw[t, pl.ds(side, q2, stride=4), :]
    pl.semaphore_wait(barrier, met)

    lane = lax.broadcasted_iota(jnp.int32, (1, LANES), 1)

    def rows_of(e):
        return rows_all if e <= 3 else s2

    def side_copy(e, side, t):
        par, rows = e % 2, rows_of(e)
        return pltpu.make_async_remote_copy(
            src_ref=sent.at[par, side, t, pl.ds(0, rows)],
            dst_ref=got.at[par, OUT_OF[side], t, pl.ds(0, rows)],
            send_sem=send_sem.at[par, side, t],
            recv_sem=recv_sem.at[par, OUT_OF[side], t],
            device_id=peer[side],
            device_id_type=MESH,
        )

    def corner_copy(e, k):
        par = e % 2
        return pltpu.make_async_remote_copy(
            src_ref=corner_out.at[par],
            dst_ref=corner_in.at[par, 3 - k],
            send_sem=csend_sem.at[par, k],
            recv_sem=crecv_sem.at[par, 3 - k],
            device_id=diag[k],
            device_id_type=MESH,
        )

    def send_corners(e, block):
        last = thirds - 1
        n0, n1 = block(NORTH, 0)[:, 0:1], block(NORTH, last)[:, LANES - 1 :]
        s0, s1 = block(SOUTH, 0)[:, 0:1], block(SOUTH, last)[:, LANES - 1 :]
        w0, w1 = block(WEST, 0)[:, 0:1], block(WEST, last)[:, LANES - 1 :]
        e0, e1 = block(EAST, 0)[:, 0:1], block(EAST, last)[:, LANES - 1 :]
        nw, ne, sw, se = n0 + w0, n1 + e0, s0 + w1, s1 + e1
        z = jnp.where(
            lane == 0, nw, jnp.where(lane == 1, ne, jnp.where(lane == 2, sw, se))
        )
        first = z[0:LANES].T[0:4]
        if z.shape[0] > s2:
            spare = jnp.zeros((2 * LANES - z.shape[0], LANES), jnp.float32)
            second = jnp.concatenate([z[LANES:], spare], axis=0).T[0:4]
        else:
            second = jnp.zeros_like(first)
        corner_out[e % 2] = jnp.concatenate([first, second], axis=0)
        for k in range(4):
            corner_copy(e, k).start()

    chunk = part.shape[2]

    def stage_a(a, j):
        d = j
        target = lax.rem(sy + d, nsy)
        return pltpu.make_async_remote_copy(
            src_ref=part.at[a, target // nx],
            dst_ref=plane_in.at[a, nsy - d],
            send_sem=asend_sem.at[a, 0],
            recv_sem=arecv_sem.at[a, 0],
            device_id=dev(target, sx),
            device_id_type=MESH,
        )

    def stage_b(a, d):
        return pltpu.make_async_remote_copy(
            src_ref=line_out.at[a],
            dst_ref=line_in.at[a, nz - d],
            send_sem=asend_sem.at[a, 1],
            recv_sem=arecv_sem.at[a, 1],
            device_id=dev(sy, lax.rem(sx + d, nz)),
            device_id_type=MESH,
        )

    def stage_c(a, d):
        return pltpu.make_async_remote_copy(
            src_ref=col_out.at[a],
            dst_ref=col_in.at[a, ny - d],
            send_sem=asend_sem.at[a, 2],
            recv_sem=arecv_sem.at[a, 2],
            device_id=dev(lax.rem(sy + d * nx, nsy), sx),
            device_id_type=MESH,
        )

    def whole(a, stage):
        buf = (plane_in, line_in, col_in)[stage]
        n = (nsy, nz, ny)[stage]
        ref = buf.at[a, pl.ds(1, n - 1)]
        return pltpu.make_async_remote_copy(
            src_ref=ref,
            dst_ref=ref,
            send_sem=asend_sem.at[a, stage],
            recv_sem=arecv_sem.at[a, stage],
            device_id=peer[EAST],
            device_id_type=MESH,
        )

    def summed(values):
        while len(values) > 1:
            values = [
                values[i] + values[i + 1] if i + 1 < len(values) else values[i]
                for i in range(0, len(values), 2)
            ]
        return values[0]

    def start_sum(a, payload):
        for j in range(ny):
            part[a, j] = payload[j * chunk : (j + 1) * chunk]
        for d in range(1, nsy):
            stage_a(a, d).start()

    def sum_b(a):
        whole(a, 0).wait_recv()
        plane_in[a, 0] = part[a, yy]
        line_out[a] = summed([plane_in[a, lax.rem(j - sy + nsy, nsy)] for j in range(nsy)])
        for d in range(1, nz):
            stage_b(a, d).start()

    def sum_c(a):
        whole(a, 1).wait_recv()
        line_in[a, 0] = line_out[a]
        col_out[a] = summed([line_in[a, lax.rem(j - sx + nz, nz)] for j in range(nz)])
        for d in range(1, ny):
            stage_c(a, d).start()

    def sum_end(a):
        whole(a, 2).wait_recv()
        col_in[a, 0] = col_out[a]
        return jnp.concatenate([col_in[a, lax.rem(j - yy + ny, ny)] for j in range(ny)], axis=0)

    for t in order:
        for side in range(4):
            side_copy(1, side, t).start()
    send_corners(1, lambda side, t: sent[1, side, t])

    def split(value, side, t, first, last):
        at = place(side, t)
        hi = value.astype(jnp.bfloat16)
        out_hi[first:last, at : at + LANES] = hi
        out_lo[first:last, at : at + LANES] = (value - hi.astype(jnp.float32)).astype(jnp.bfloat16)

    for t in order:
        for side in range(4):
            split(src_ref[side, t], side, t, 0, s2)

    for t in order:
        pro_load[t].wait()
        for side in range(4):
            at = place(side, t)
            lhs[s2:rows_all, at : at + LANES] = pro_raw[t, pl.ds(side, q2, stride=4), :].astype(
                jnp.bfloat16
            )

    rows_i = lax.broadcasted_iota(jnp.int32, (2 * LANES, 2 * LANES), 0)
    cols_i = lax.broadcasted_iota(jnp.int32, (2 * LANES, 2 * LANES), 1)
    wanted = jnp.where(rows_i < LANES, 2 * rows_i, 2 * (rows_i - LANES) + 1)
    chosen = jnp.where(cols_i == wanted, 1.0, 0.0).astype(jnp.bfloat16)
    for b in range(blocks):
        loads[b].wait()
        parted = dot(chosen, raw[2 * LANES * b : 2 * LANES * (b + 1)], ((1,), (0,)))
        parted = parted.astype(jnp.bfloat16)
        for side in range(4):
            h, k = side // 2, 2 * (side % 2) * LANES
            for t in range(thirds):
                at = side * cells + t * LANES
                row = place(b // thirds, b % thirds)
                for c in (0, 1):
                    table[t, h, row : row + LANES, k + c * LANES : k + (c + 1) * LANES] = parted[
                        c * LANES : (c + 1) * LANES, at : at + LANES
                    ]

    def restrict(first, last):
        hi, lo = out_hi[first:last], out_lo[first:last]
        half = (last - first) // 2
        both = dot(res_split[...], hi, ((1,), (1,)))
        rest = dot(res_split[0:q2], lo, ((1,), (1,)))
        u = both[0:q2] + both[q2:] + rest
        return u[0:half_q] + turned(u[half_q:], half)

    def coarse(total):
        stacked = jnp.concatenate([total, turned(total, half_s)], axis=0)
        coef = dot(inv_ref[...], stacked, ((0,), (0,)), HIGH)
        return coef

    def stack_of(coef):
        return jnp.concatenate([coef, turned(coef, half_s)], axis=0)

    def lifted(coef, k, first=0, last=depth):
        fix[:, first:last] = dot(stack_of(coef), lift[k, :, first:last], ((0,), (0,)), HIGH)

    def corner_columns(e):
        par, rows = e % 2, rows_of(e)
        for k in range(4):
            corner_copy(e, k).wait_recv()
        tile = []
        for base in (0, 4) if rows > s2 else (0,):
            for k in range(4):
                row = corner_in[par, k, base + 3 - k : base + 4 - k]
                tile.append(jnp.where(has_diag[k], 0.5 * row, 0.0))
        spare = jnp.zeros((LANES - len(tile), LANES), jnp.float32)
        flat = jnp.concatenate([*tile, spare], axis=0).T
        cols = flat[:, 0:4]
        if rows > s2:
            cols = jnp.concatenate([cols, flat[0:q2, 4:8]], axis=0)
        nw, ne, sw, se = (cols[:, k : k + 1] for k in range(4))
        return {NORTH: (nw, ne), SOUTH: (sw, se), WEST: (nw, sw), EAST: (ne, se)}

    def receive(e, some, fixed):
        par, rows = e % 2, rows_of(e)
        first, last = place(0, some[0]), place(0, some[-1]) + 4 * LANES
        ends = corner_columns(e) if 0 in some else None

        def incoming(side, t, first, last):
            value = jnp.where(has[side], got[par, side, t, first:last], 0.0)
            if t == 0:
                value += jnp.where(lane == 0, ends[side][0][first:last], 0.0)
            if t == thirds - 1:
                value += jnp.where(lane == LANES - 1, ends[side][1][first:last], 0.0)
            return value

        for t in some:
            for side in range(4):
                side_copy(e, OUT_OF[side], t).wait_recv()
                if rows > s2:
                    at = place(side, t)
                    extra = incoming(side, t, s2, rows)
                    hi = extra.astype(jnp.bfloat16)
                    if e == 1:
                        res_split[0:q2, at : at + LANES] = hi
                        res_split[q2:, at : at + LANES] = (extra - hi.astype(jnp.float32)).astype(
                            jnp.bfloat16
                        )
                    else:
                        lift[e - 2, :, at : at + LANES] = extra
                    if e == 2:
                        lhs[s2:, at : at + LANES] = hi
        if e == 3:
            lifted(fixed, 1, first, last)
        for t in some:
            for side in range(4):
                at = place(side, t)
                top = incoming(side, t, 0, s2)
                if fixed is not None:
                    top += fix[:, at : at + LANES]
                if e == ITERS:
                    last_sum[:, at : at + LANES] = top
                else:
                    lhs[0:s2, at : at + LANES] = top.astype(jnp.bfloat16)

    def sends_done(e):
        for t in order:
            for side in range(4):
                side_copy(e, side, t).wait_send()
        for k in range(4):
            corner_copy(e, k).wait_send()

    def multiply_early(e):
        rows = rows_all if e in (2, 3) else s2
        for t in order:
            for h in (0, 1):
                acc[t, h, 0:rows] = dot(lhs[0:rows, 0:early], table[t, h, 0:early], ((1,), (0,)))

    def multiply_late(e):
        rows, par = rows_of(e), e % 2
        if e >= 3:
            sends_done(e - 2)

        for t in (*order, None):
            if t == order[-1]:
                send_corners(e, lambda side, t: sent[par, side, t, 0:rows])
            if t is None:
                break
            for h in (0, 1):
                product = acc[t, h, 0:rows] + dot(
                    lhs[0:rows, early:], table[t, h, early:], ((1,), (0,))
                )
                for k in (0, 1):
                    side = 2 * h + k
                    re = product[:, 2 * k * LANES : (2 * k + 1) * LANES]
                    im = product[:, (2 * k + 1) * LANES : (2 * k + 2) * LANES]
                    a, b = half_s, s2
                    out_re = re[0:a] - im[a:b] + src_ref[side, t, 0:a]
                    out_im = im[0:a] + re[a:b] + src_ref[side, t, a:b]
                    sent[par, side, t, 0:a] = out_re
                    sent[par, side, t, a:b] = out_im
                    if e < ITERS:
                        split(out_re, side, t, 0, a)
                        split(out_im, side, t, a, b)
                    if rows > s2:
                        a, b = s2 + half_q, s2 + q2
                        out_re = re[s2:a] - im[a:b]
                        out_im = im[s2:a] + re[a:b]
                        sent[par, side, t, s2:a] = out_re
                        sent[par, side, t, a:b] = out_im
                        split(out_re, side, t, s2, a)
                        split(out_im, side, t, a, b)
                    side_copy(e, side, t).start()

    coef, share = {}, {}

    def finish(j):
        total = sum_end(j)
        if j == 2:
            share[0] = sum_end(0)[:, 0:q2]
        if j == 3:
            share[1] = sum_end(ITERS)[:, 0:q2]
        for k in (0, 1):
            if j - 1 - k >= 1:
                total += dot(share[k], stack_of(coef[j - 1 - k]), ((1,), (0,)), HIGH)
        coef[j] = coarse(total)

    def lifted_rows():
        half = restrict(s2, rows_all)
        return jnp.concatenate([half, jnp.zeros((half_q, LANES - q2), jnp.float32)], axis=1)

    for i in range(1, ITERS):
        receive(i, order[:-1], coef.get(i - 2))
        multiply_early(i + 1)
        receive(i, order[-1:], coef.get(i - 2))
        if i == 1:
            start_sum(1, restrict(0, s2))
        multiply_late(i + 1)
        if i >= 2:
            sum_c(i - 1)
        if i == 3:
            sum_c(0)
        if i == 4:
            sum_c(ITERS)
        sum_b(i)
        if i == 2:
            sum_b(0)
        if i == 3:
            sum_b(ITERS)
        if i < ITERS - 1:
            start_sum(i + 1, restrict(0, s2))
        if i == 1:
            start_sum(0, lifted_rows())
        if i == 2:
            start_sum(ITERS, lifted_rows())
        if i >= 2:
            finish(i - 1)
        if i >= 3:
            lifted(coef[i - 1], 1)

    receive(ITERS, order[:-1], coef[ITERS - 2])
    receive(ITERS, order[-1:], coef[ITERS - 2])
    sum_c(ITERS - 1)
    finish(ITERS - 1)
    lifted(coef[ITERS - 1], 0)
    flat_out = out_hbm.reshape(4 * s2, cells)
    stores = [
        pltpu.make_async_copy(
            src_raw.at[t], flat_out.at[:, pl.ds(t * LANES, LANES)], load_sem.at[0, t]
        )
        for t in range(thirds)
    ]
    for t in range(thirds):
        for side in range(4):
            at = place(side, t)
            src_raw[t, pl.ds(side, s2, stride=4), :] = (
                last_sum[:, at : at + LANES] + fix[:, at : at + LANES]
            )
        stores[t].start()
    coef_ref[0] = coef[ITERS - 1][:, 0:half_s]
    coef_ref[1] = coef[ITERS - 1][:, half_s:]
    sends_done(ITERS - 1)
    sends_done(ITERS)
    for a in range(ITERS + 1):
        for stage in range(3):
            whole(a, stage).wait_send()
    for t in range(thirds):
        stores[t].wait()


def solution(mesh):
    nsy, nz = mesh.shape["sy"], mesh.shape["sx"]
    nx = 4
    ny = nsy // nx

    def per_device(interface_map, source_trace, restriction, prolongation, coarse_inverse):
        src_count, cells = source_trace.shape[3], source_trace.shape[5]
        width = restriction.shape[3]
        thirds = cells // LANES
        s2, q2 = 2 * src_count, 2 * width
        rows = s2 + q2
        depth = 4 * cells
        dims = (ny, nx, nz, s2, q2, thirds)
        chunk = width // ny
        vmem = pl.BlockSpec(memory_space=pltpu.VMEM)
        hbm = pl.BlockSpec(memory_space=pl.ANY)
        traces, coef = pl.pallas_call(
            functools.partial(kernel, dims),
            out_shape=(
                jax.ShapeDtypeStruct((2, src_count, 4, cells), jnp.float32),
                jax.ShapeDtypeStruct((2, width, src_count), jnp.float32),
            ),
            in_specs=[hbm, hbm, hbm, hbm, vmem],
            out_specs=(hbm, vmem),
            scratch_shapes=[
                pltpu.VMEM((2 * depth, depth), jnp.bfloat16),
                pltpu.VMEM((thirds, 4 * s2, LANES), jnp.float32),
                pltpu.VMEM((thirds, 4 * q2, LANES), jnp.float32),
                pltpu.VMEM((thirds, 4 * q2, LANES), jnp.float32),
                pltpu.VMEM((4, thirds, s2, LANES), jnp.float32),
                pltpu.VMEM((thirds, 2, depth, 4 * LANES), jnp.bfloat16),
                pltpu.VMEM((rows, depth), jnp.bfloat16),
                pltpu.VMEM((thirds, 2, rows, 4 * LANES), jnp.float32),
                pltpu.VMEM((rows, depth), jnp.bfloat16),
                pltpu.VMEM((rows, depth), jnp.bfloat16),
                pltpu.VMEM((2, 4, thirds, rows, LANES), jnp.float32),
                pltpu.VMEM((2, 4, thirds, rows, LANES), jnp.float32),
                pltpu.VMEM((2, q2, depth), jnp.float32),
                pltpu.VMEM((2 * q2, depth), jnp.bfloat16),
                pltpu.VMEM((2, 8, LANES), jnp.float32),
                pltpu.VMEM((2, 4, 8, LANES), jnp.float32),
                pltpu.VMEM((ITERS + 1, ny, chunk, LANES), jnp.float32),
                pltpu.VMEM((ITERS + 1, nsy, chunk, LANES), jnp.float32),
                pltpu.VMEM((ITERS + 1, chunk, LANES), jnp.float32),
                pltpu.VMEM((ITERS + 1, nz, chunk, LANES), jnp.float32),
                pltpu.VMEM((ITERS + 1, chunk, LANES), jnp.float32),
                pltpu.VMEM((ITERS + 1, ny, chunk, LANES), jnp.float32),
                pltpu.VMEM((s2, depth), jnp.float32),
                pltpu.VMEM((s2, depth), jnp.float32),
                pltpu.SemaphoreType.DMA((depth // LANES,)),
                pltpu.SemaphoreType.DMA((3, thirds)),
                pltpu.SemaphoreType.DMA((2, 4, thirds)),
                pltpu.SemaphoreType.DMA((2, 4, thirds)),
                pltpu.SemaphoreType.DMA((2, 4)),
                pltpu.SemaphoreType.DMA((2, 4)),
                pltpu.SemaphoreType.DMA((ITERS + 1, 3)),
                pltpu.SemaphoreType.DMA((ITERS + 1, 3)),
            ],
            compiler_params=pltpu.CompilerParams(
                collective_id=0, has_side_effects=True, vmem_limit_bytes=60 * 1024 * 1024
            ),
        )(
            interface_map.reshape(depth, 2, depth),
            source_trace.reshape(2, src_count, 4, cells),
            restriction.reshape(2, width, 4, cells),
            prolongation.reshape(2, width, 4, cells),
            coarse_inverse.reshape(q2, width),
        )
        return traces.reshape(source_trace.shape), coef.transpose(0, 2, 1)

    where = P(("wl", "sy"), "sx", None, None, None, None)
    return jax.shard_map(
        per_device,
        mesh=mesh,
        in_specs=(P(("wl", "sy"), "sx", None, None, None), where, where, where, P("wl", None, None)),
        out_specs=(where, P("wl", None, None)),
        check_vma=False,
    )
```

```python
import functools

import jax
import jax.numpy as jnp
from jax import lax
from jax.experimental import pallas as pl
from jax.experimental.pallas import tpu as pltpu
from jax.sharding import PartitionSpec as P

ITERS = 6
LANES = 128
MESH = pl.DeviceIdType.MESH
HIGH = lax.Precision.HIGHEST
NORTH, SOUTH, WEST, EAST = 0, 1, 2, 3
OUT_OF = {NORTH: SOUTH, SOUTH: NORTH, WEST: EAST, EAST: WEST}


def dot(a, b, contract, precision=None):
    return lax.dot_general(
        a, b, (contract, ((), ())), preferred_element_type=jnp.float32, precision=precision
    )


def turned(pair, half):
    return jnp.concatenate([-pair[:, half:], pair[:, :half]], axis=1)


def kernel(
    dims,
    map_hbm,
    src_hbm,
    res_hbm,
    pro_hbm,
    inv_ref,
    out_hbm,
    coef_ref,
    raw,
    src_raw,
    res_raw,
    pro_raw,
    src_ref,
    table,
    lhs,
    acc,
    src_hi,
    src_lo,
    out_hi,
    out_lo,
    sent,
    got,
    lift,
    res_split,
    corner_out,
    corner_in,
    part,
    plane_in,
    line_out,
    line_in,
    col_out,
    col_in,
    fix,
    last_sum,
    map_sem,
    load_sem,
    send_sem,
    recv_sem,
    wsend_sem,
    wrecv_sem,
    csend_sem,
    crecv_sem,
    asend_sem,
    arecv_sem,
):
    ny, nx, nz, s2, q2, thirds = dims
    cells = thirds * LANES
    nsy = ny * nx
    rows_all = s2 + q2
    half_s, half_q = s2 // 2, q2 // 2
    sy, sx = lax.axis_index("sy"), lax.axis_index("sx")
    wl = lax.axis_index("wl")
    yy = sy // nx

    def dev(row, col):
        return (row, col, wl)

    def place(side, t):
        return (order.index(t) * 4 + side) * LANES

    up, down = lax.rem(sy + nsy - 1, nsy), lax.rem(sy + 1, nsy)
    left, right = lax.rem(sx + nz - 1, nz), lax.rem(sx + 1, nz)
    peer = {NORTH: dev(up, sx), SOUTH: dev(down, sx), WEST: dev(sy, left), EAST: dev(sy, right)}
    diag = (dev(up, left), dev(up, right), dev(down, left), dev(down, right))
    has = {NORTH: sy > 0, SOUTH: sy < nsy - 1, WEST: sx > 0, EAST: sx < nz - 1}
    has_diag = (
        (sy > 0) & (sx > 0),
        (sy > 0) & (sx < nz - 1),
        (sy < nsy - 1) & (sx > 0),
        (sy < nsy - 1) & (sx < nz - 1),
    )

    depth = 4 * cells
    order = (0, *range(2, thirds), 1)
    early = 4 * LANES * (thirds - 1)
    blocks = depth // LANES
    flat_map = map_hbm.reshape(2 * depth, depth)
    loads = [
        pltpu.make_async_copy(
            flat_map.at[pl.ds(2 * LANES * b, 2 * LANES)],
            raw.at[pl.ds(2 * LANES * b, 2 * LANES)],
            map_sem.at[b],
        )
        for b in range(blocks)
    ]
    flat_src = src_hbm.reshape(4 * s2, cells)
    flat_pro = pro_hbm.reshape(4 * q2, cells)
    flat_res = res_hbm.reshape(4 * q2, cells)

    def third(flat, held, which):
        return [
            pltpu.make_async_copy(
                flat.at[:, pl.ds(t * LANES, LANES)], held.at[t], load_sem.at[which, t]
            )
            for t in range(thirds)
        ]

    src_load = third(flat_src, src_raw, 0)
    pro_load = third(flat_pro, pro_raw, 1)
    res_load = third(flat_res, res_raw, 2)
    for copy in (*src_load, *pro_load, *res_load):
        copy.start()
    for b in range(blocks):
        loads[b].start()

    barrier = pltpu.get_barrier_semaphore()
    met = 0
    for target in (*peer.values(), *diag):
        pl.semaphore_signal(barrier, inc=1, device_id=target, device_id_type=MESH)
        met += 1
    for d in range(1, nsy):
        target = dev(lax.rem(sy + d, nsy), sx)
        pl.semaphore_signal(barrier, inc=1, device_id=target, device_id_type=MESH)
        met += 1
    for d in range(1, nz):
        target = dev(sy, lax.rem(sx + d, nz))
        pl.semaphore_signal(barrier, inc=1, device_id=target, device_id_type=MESH)
        met += 1
    for t in order:
        src_load[t].wait()
        res_load[t].wait()
        for side in range(4):
            at = place(side, t)
            value = src_raw[t, pl.ds(side, s2, stride=4), :]
            src_ref[side, t] = value
            sent[1, side, t, 0:s2] = value
            sent[1, side, t, s2:] = res_raw[t, pl.ds(side, q2, stride=4), :]
    pl.semaphore_wait(barrier, met)

    lane = lax.broadcasted_iota(jnp.int32, (1, LANES), 1)

    def rows_of(e):
        return rows_all if e in (2, 3) else s2

    def side_copy(e, side, t):
        par, rows = e % 2, rows_of(e)
        return pltpu.make_async_remote_copy(
            src_ref=sent.at[par, side, t, pl.ds(0, rows)],
            dst_ref=got.at[par, OUT_OF[side], t, pl.ds(0, rows)],
            send_sem=send_sem.at[par, side, t],
            recv_sem=recv_sem.at[par, OUT_OF[side], t],
            device_id=peer[side],
            device_id_type=MESH,
        )

    def weight_copy(side, t):
        return pltpu.make_async_remote_copy(
            src_ref=sent.at[1, side, t, pl.ds(s2, q2)],
            dst_ref=got.at[1, OUT_OF[side], t, pl.ds(s2, q2)],
            send_sem=wsend_sem.at[side, t],
            recv_sem=wrecv_sem.at[OUT_OF[side], t],
            device_id=peer[side],
            device_id_type=MESH,
        )

    def corner_copy(e, k):
        par = e % 2
        return pltpu.make_async_remote_copy(
            src_ref=corner_out.at[par],
            dst_ref=corner_in.at[par, 3 - k],
            send_sem=csend_sem.at[par, k],
            recv_sem=crecv_sem.at[par, 3 - k],
            device_id=diag[k],
            device_id_type=MESH,
        )

    def send_corners(e, block):
        last = thirds - 1
        n0, n1 = block(NORTH, 0)[:, 0:1], block(NORTH, last)[:, LANES - 1 :]
        s0, s1 = block(SOUTH, 0)[:, 0:1], block(SOUTH, last)[:, LANES - 1 :]
        w0, w1 = block(WEST, 0)[:, 0:1], block(WEST, last)[:, LANES - 1 :]
        e0, e1 = block(EAST, 0)[:, 0:1], block(EAST, last)[:, LANES - 1 :]
        nw, ne, sw, se = n0 + w0, n1 + e0, s0 + w1, s1 + e1
        z = jnp.where(
            lane == 0, nw, jnp.where(lane == 1, ne, jnp.where(lane == 2, sw, se))
        )
        first = z[0:LANES].T[0:4]
        if z.shape[0] > s2:
            spare = jnp.zeros((2 * LANES - z.shape[0], LANES), jnp.float32)
            second = jnp.concatenate([z[LANES:], spare], axis=0).T[0:4]
        else:
            second = jnp.zeros_like(first)
        corner_out[e % 2] = jnp.concatenate([first, second], axis=0)
        for k in range(4):
            corner_copy(e, k).start()

    chunk = part.shape[2]

    def stage_a(a, j):
        d = j
        target = lax.rem(sy + d, nsy)
        return pltpu.make_async_remote_copy(
            src_ref=part.at[a, target // nx],
            dst_ref=plane_in.at[a, nsy - d],
            send_sem=asend_sem.at[a, 0],
            recv_sem=arecv_sem.at[a, 0],
            device_id=dev(target, sx),
            device_id_type=MESH,
        )

    def stage_b(a, d):
        return pltpu.make_async_remote_copy(
            src_ref=line_out.at[a],
            dst_ref=line_in.at[a, nz - d],
            send_sem=asend_sem.at[a, 1],
            recv_sem=arecv_sem.at[a, 1],
            device_id=dev(sy, lax.rem(sx + d, nz)),
            device_id_type=MESH,
        )

    def stage_c(a, d):
        return pltpu.make_async_remote_copy(
            src_ref=col_out.at[a],
            dst_ref=col_in.at[a, ny - d],
            send_sem=asend_sem.at[a, 2],
            recv_sem=arecv_sem.at[a, 2],
            device_id=dev(lax.rem(sy + d * nx, nsy), sx),
            device_id_type=MESH,
        )

    def whole(a, stage):
        buf = (plane_in, line_in, col_in)[stage]
        n = (nsy, nz, ny)[stage]
        ref = buf.at[a, pl.ds(1, n - 1)]
        return pltpu.make_async_remote_copy(
            src_ref=ref,
            dst_ref=ref,
            send_sem=asend_sem.at[a, stage],
            recv_sem=arecv_sem.at[a, stage],
            device_id=peer[EAST],
            device_id_type=MESH,
        )

    def summed(values):
        while len(values) > 1:
            values = [
                values[i] + values[i + 1] if i + 1 < len(values) else values[i]
                for i in range(0, len(values), 2)
            ]
        return values[0]

    def start_sum(a, payload):
        for j in range(ny):
            part[a, j] = payload[j * chunk : (j + 1) * chunk]
        for d in range(1, nsy):
            stage_a(a, d).start()

    def sum_b(a):
        whole(a, 0).wait_recv()
        plane_in[a, 0] = part[a, yy]
        line_out[a] = summed([plane_in[a, lax.rem(j - sy + nsy, nsy)] for j in range(nsy)])
        for d in range(1, nz):
            stage_b(a, d).start()

    def sum_c(a):
        whole(a, 1).wait_recv()
        line_in[a, 0] = line_out[a]
        col_out[a] = summed([line_in[a, lax.rem(j - sx + nz, nz)] for j in range(nz)])
        for d in range(1, ny):
            stage_c(a, d).start()

    def sum_end(a):
        whole(a, 2).wait_recv()
        col_in[a, 0] = col_out[a]
        return jnp.concatenate([col_in[a, lax.rem(j - yy + ny, ny)] for j in range(ny)], axis=0)

    send_corners(1, lambda side, t: sent[1, side, t])
    for t in order:
        for side in range(4):
            side_copy(1, side, t).start()
    for t in order:
        for side in range(4):
            weight_copy(side, t).start()

    def split(value, side, t, first, last):
        at = place(side, t)
        hi = value.astype(jnp.bfloat16)
        out_hi[first:last, at : at + LANES] = hi
        out_lo[first:last, at : at + LANES] = (value - hi.astype(jnp.float32)).astype(jnp.bfloat16)

    for t in order:
        for side in range(4):
            at, value = place(side, t), src_ref[side, t]
            hi = value.astype(jnp.bfloat16)
            src_hi[:, at : at + LANES] = hi
            src_lo[:, at : at + LANES] = (value - hi.astype(jnp.float32)).astype(jnp.bfloat16)

    for t in order:
        pro_load[t].wait()
        for side in range(4):
            at = place(side, t)
            lhs[s2:rows_all, at : at + LANES] = pro_raw[t, pl.ds(side, q2, stride=4), :].astype(
                jnp.bfloat16
            )

    rows_i = lax.broadcasted_iota(jnp.int32, (2 * LANES, 2 * LANES), 0)
    cols_i = lax.broadcasted_iota(jnp.int32, (2 * LANES, 2 * LANES), 1)
    wanted = jnp.where(rows_i < LANES, 2 * rows_i, 2 * (rows_i - LANES) + 1)
    chosen = jnp.where(cols_i == wanted, 1.0, 0.0).astype(jnp.bfloat16)
    for b in range(blocks):
        loads[b].wait()
        parted = dot(chosen, raw[2 * LANES * b : 2 * LANES * (b + 1)], ((1,), (0,)))
        parted = parted.astype(jnp.bfloat16)
        for side in range(4):
            h, k = side // 2, 2 * (side % 2) * LANES
            for t in range(thirds):
                at = side * cells + t * LANES
                row = place(b // thirds, b % thirds)
                for c in (0, 1):
                    table[t, h, row : row + LANES, k + c * LANES : k + (c + 1) * LANES] = parted[
                        c * LANES : (c + 1) * LANES, at : at + LANES
                    ]

    def restrict(first, last):
        return restricted(out_hi[first:last], out_lo[first:last])

    def restricted(hi, lo):
        half = hi.shape[0] // 2
        both = dot(res_split[...], hi, ((1,), (1,)))
        rest = dot(res_split[0:q2], lo, ((1,), (1,)))
        u = both[0:q2] + both[q2:] + rest
        return u[0:half_q] + turned(u[half_q:], half)

    def coarse(total):
        stacked = jnp.concatenate([total, turned(total, half_s)], axis=0)
        coef = dot(inv_ref[...], stacked, ((0,), (0,)), HIGH)
        return coef

    def stack_of(coef):
        return jnp.concatenate([coef, turned(coef, half_s)], axis=0)

    def lifted(coef, k, first=0, last=depth):
        stack = stack_of(coef)
        hi = stack.astype(jnp.bfloat16)
        rest = (stack - hi.astype(jnp.float32)).astype(jnp.bfloat16)
        three = jnp.concatenate([hi, hi, rest], axis=0)
        fix[:, first:last] = dot(three, lift[k, :, first:last], ((0,), (0,)))

    def corner_columns(e):
        par, rows = e % 2, rows_of(e)
        for k in range(4):
            corner_copy(e, k).wait_recv()
        tile = []
        for base in (0, 4) if e <= 3 else (0,):
            for k in range(4):
                row = corner_in[par, k, base + 3 - k : base + 4 - k]
                tile.append(jnp.where(has_diag[k], 0.5 * row, 0.0))
        spare = jnp.zeros((LANES - len(tile), LANES), jnp.float32)
        flat = jnp.concatenate([*tile, spare], axis=0).T
        cols = flat[:, 0:4]
        if e <= 3:
            cols = jnp.concatenate([cols, flat[0:q2, 4:8]], axis=0)
        nw, ne, sw, se = (cols[:, k : k + 1] for k in range(4))
        return {NORTH: (nw, ne), SOUTH: (sw, se), WEST: (nw, sw), EAST: (ne, se)}

    def arrived(par, ends, side, t, first, last):
        value = jnp.where(has[side], got[par, side, t, first:last], 0.0)
        if t == 0:
            value += jnp.where(lane == 0, ends[side][0][first:last], 0.0)
        if t == thirds - 1:
            value += jnp.where(lane == LANES - 1, ends[side][1][first:last], 0.0)
        return value

    def receive_weights(ends):
        for t in order:
            for side in range(4):
                weight_copy(OUT_OF[side], t).wait_recv()
                at = place(side, t)
                extra = arrived(1, ends, side, t, s2, rows_all)
                hi = extra.astype(jnp.bfloat16)
                res_split[0:q2, at : at + LANES] = hi
                res_split[q2:, at : at + LANES] = (extra - hi.astype(jnp.float32)).astype(
                    jnp.bfloat16
                )
        for t in order:
            for side in range(4):
                weight_copy(side, t).wait_send()

    def receive(e, some, fixed, ends=None):
        par, rows = e % 2, rows_of(e)
        first, last = place(0, some[0]), place(0, some[-1]) + 4 * LANES
        ends = corner_columns(e) if ends is None else ends

        def incoming(side, t, first, last):
            return arrived(par, ends, side, t, first, last)

        for t in some:
            for side in range(4):
                side_copy(e, OUT_OF[side], t).wait_recv()
                if rows > s2:
                    at = place(side, t)
                    extra = incoming(side, t, s2, rows)
                    hi = extra.astype(jnp.bfloat16)
                    rest = (extra - hi.astype(jnp.float32)).astype(jnp.bfloat16)
                    lift[e - 2, 0:q2, at : at + LANES] = hi
                    lift[e - 2, q2 : 2 * q2, at : at + LANES] = rest
                    lift[e - 2, 2 * q2 :, at : at + LANES] = hi
                    if e == 2:
                        lhs[s2:, at : at + LANES] = hi
        if e == 3:
            lifted(fixed, 1, first, last)
        for t in some:
            for side in range(4):
                at = place(side, t)
                top = incoming(side, t, 0, s2)
                if fixed is not None:
                    top += fix[:, at : at + LANES]
                if e == ITERS:
                    last_sum[:, at : at + LANES] = top
                else:
                    lhs[0:s2, at : at + LANES] = top.astype(jnp.bfloat16)
        return ends

    def sends_done(e):
        for t in order:
            for side in range(4):
                side_copy(e, side, t).wait_send()
        for k in range(4):
            corner_copy(e, k).wait_send()

    def multiply_early(e):
        rows = rows_all if e in (2, 3) else s2
        for t in order:
            for h in (0, 1):
                acc[t, h, 0:rows] = dot(lhs[0:rows, 0:early], table[t, h, 0:early], ((1,), (0,)))

    def multiply_late(e):
        rows, par = rows_of(e), e % 2
        if e >= 3:
            sends_done(e - 2)

        for t in (*order, None):
            if t == order[-1]:
                send_corners(e, lambda side, t: sent[par, side, t, 0:rows])
            if t is None:
                break
            for h in (0, 1):
                product = acc[t, h, 0:rows] + dot(
                    lhs[0:rows, early:], table[t, h, early:], ((1,), (0,))
                )
                for k in (0, 1):
                    side = 2 * h + k
                    re = product[:, 2 * k * LANES : (2 * k + 1) * LANES]
                    im = product[:, (2 * k + 1) * LANES : (2 * k + 2) * LANES]
                    a, b = half_s, s2
                    out_re = re[0:a] - im[a:b] + src_ref[side, t, 0:a]
                    out_im = im[0:a] + re[a:b] + src_ref[side, t, a:b]
                    sent[par, side, t, 0:a] = out_re
                    sent[par, side, t, a:b] = out_im
                    if e < ITERS:
                        split(out_re, side, t, 0, a)
                        split(out_im, side, t, a, b)
                    if rows > s2:
                        a, b = s2 + half_q, s2 + q2
                        out_re = re[s2:a] - im[a:b]
                        out_im = im[s2:a] + re[a:b]
                        sent[par, side, t, s2:a] = out_re
                        sent[par, side, t, a:b] = out_im
                        split(out_re, side, t, s2, a)
                        split(out_im, side, t, a, b)
                    side_copy(e, side, t).start()

    coef, share = {}, {}

    def finish(j):
        total = sum_end(j)
        if j == 2:
            share[0] = sum_end(0)[:, 0:q2]
        if j == 3:
            share[1] = sum_end(ITERS)[:, 0:q2]
        for k in (0, 1):
            if j - 1 - k >= 1:
                total += dot(share[k], stack_of(coef[j - 1 - k]), ((1,), (0,)), HIGH)
        coef[j] = coarse(total)

    def lifted_rows():
        half = restrict(s2, rows_all)
        return jnp.concatenate([half, jnp.zeros((half_q, LANES - q2), jnp.float32)], axis=1)

    for i in range(1, ITERS):
        ends = receive(i, order[:-1], coef.get(i - 2))
        multiply_early(i + 1)
        if i >= 2:
            sum_b(i)
        if i == 2:
            sum_b(0)
        if i == 3:
            sum_b(ITERS)
        receive(i, order[-1:], coef.get(i - 2), ends)
        if i == 1:
            receive_weights(ends)
            start_sum(1, restricted(src_hi[...], src_lo[...]))
        multiply_late(i + 1)
        if i == 2:
            sum_c(1)
        if i < ITERS - 1:
            start_sum(i + 1, restrict(0, s2))
        if i == 1:
            start_sum(0, lifted_rows())
            sum_b(1)
        if i == 2:
            start_sum(ITERS, lifted_rows())
        if i >= 3:
            finish(i - 1)
            lifted(coef[i - 1], 1)
        if i >= 2:
            sum_c(i)
        if i == 2:
            sum_c(0)
            finish(1)
        if i == 3:
            sum_c(ITERS)

    ends = receive(ITERS, order[:-1], coef[ITERS - 2])
    receive(ITERS, order[-1:], coef[ITERS - 2], ends)
    finish(ITERS - 1)
    lifted(coef[ITERS - 1], 0)
    flat_out = out_hbm.reshape(4 * s2, cells)
    stores = [
        pltpu.make_async_copy(
            src_raw.at[t], flat_out.at[:, pl.ds(t * LANES, LANES)], load_sem.at[0, t]
        )
        for t in range(thirds)
    ]
    for t in range(thirds):
        for side in range(4):
            at = place(side, t)
            src_raw[t, pl.ds(side, s2, stride=4), :] = (
                last_sum[:, at : at + LANES] + fix[:, at : at + LANES]
            )
        stores[t].start()
    coef_ref[0] = coef[ITERS - 1][:, 0:half_s]
    coef_ref[1] = coef[ITERS - 1][:, half_s:]
    sends_done(ITERS - 1)
    sends_done(ITERS)
    for a in range(ITERS + 1):
        for stage in range(3):
            whole(a, stage).wait_send()
    for t in range(thirds):
        stores[t].wait()


def solution(mesh):
    nsy, nz = mesh.shape["sy"], mesh.shape["sx"]
    nx = 4
    ny = nsy // nx

    def per_device(interface_map, source_trace, restriction, prolongation, coarse_inverse):
        src_count, cells = source_trace.shape[3], source_trace.shape[5]
        width = restriction.shape[3]
        thirds = cells // LANES
        s2, q2 = 2 * src_count, 2 * width
        rows = s2 + q2
        depth = 4 * cells
        dims = (ny, nx, nz, s2, q2, thirds)
        chunk = width // ny
        vmem = pl.BlockSpec(memory_space=pltpu.VMEM)
        hbm = pl.BlockSpec(memory_space=pl.ANY)
        traces, coef = pl.pallas_call(
            functools.partial(kernel, dims),
            out_shape=(
                jax.ShapeDtypeStruct((2, src_count, 4, cells), jnp.float32),
                jax.ShapeDtypeStruct((2, width, src_count), jnp.float32),
            ),
            in_specs=[hbm, hbm, hbm, hbm, vmem],
            out_specs=(hbm, vmem),
            scratch_shapes=[
                pltpu.VMEM((2 * depth, depth), jnp.bfloat16),
                pltpu.VMEM((thirds, 4 * s2, LANES), jnp.float32),
                pltpu.VMEM((thirds, 4 * q2, LANES), jnp.float32),
                pltpu.VMEM((thirds, 4 * q2, LANES), jnp.float32),
                pltpu.VMEM((4, thirds, s2, LANES), jnp.float32),
                pltpu.VMEM((thirds, 2, depth, 4 * LANES), jnp.bfloat16),
                pltpu.VMEM((rows, depth), jnp.bfloat16),
                pltpu.VMEM((thirds, 2, rows, 4 * LANES), jnp.float32),
                pltpu.VMEM((s2, depth), jnp.bfloat16),
                pltpu.VMEM((s2, depth), jnp.bfloat16),
                pltpu.VMEM((rows, depth), jnp.bfloat16),
                pltpu.VMEM((rows, depth), jnp.bfloat16),
                pltpu.VMEM((2, 4, thirds, rows, LANES), jnp.float32),
                pltpu.VMEM((2, 4, thirds, rows, LANES), jnp.float32),
                pltpu.VMEM((2, 3 * q2, depth), jnp.bfloat16),
                pltpu.VMEM((2 * q2, depth), jnp.bfloat16),
                pltpu.VMEM((2, 8, LANES), jnp.float32),
                pltpu.VMEM((2, 4, 8, LANES), jnp.float32),
                pltpu.VMEM((ITERS + 1, ny, chunk, LANES), jnp.float32),
                pltpu.VMEM((ITERS + 1, nsy, chunk, LANES), jnp.float32),
                pltpu.VMEM((ITERS + 1, chunk, LANES), jnp.float32),
                pltpu.VMEM((ITERS + 1, nz, chunk, LANES), jnp.float32),
                pltpu.VMEM((ITERS + 1, chunk, LANES), jnp.float32),
                pltpu.VMEM((ITERS + 1, ny, chunk, LANES), jnp.float32),
                pltpu.VMEM((s2, depth), jnp.float32),
                pltpu.VMEM((s2, depth), jnp.float32),
                pltpu.SemaphoreType.DMA((depth // LANES,)),
                pltpu.SemaphoreType.DMA((3, thirds)),
                pltpu.SemaphoreType.DMA((2, 4, thirds)),
                pltpu.SemaphoreType.DMA((2, 4, thirds)),
                pltpu.SemaphoreType.DMA((4, thirds)),
                pltpu.SemaphoreType.DMA((4, thirds)),
                pltpu.SemaphoreType.DMA((2, 4)),
                pltpu.SemaphoreType.DMA((2, 4)),
                pltpu.SemaphoreType.DMA((ITERS + 1, 3)),
                pltpu.SemaphoreType.DMA((ITERS + 1, 3)),
            ],
            compiler_params=pltpu.CompilerParams(
                collective_id=0, has_side_effects=True, vmem_limit_bytes=60 * 1024 * 1024
            ),
        )(
            interface_map.reshape(depth, 2, depth),
            source_trace.reshape(2, src_count, 4, cells),
            restriction.reshape(2, width, 4, cells),
            prolongation.reshape(2, width, 4, cells),
            coarse_inverse.reshape(q2, width),
        )
        return traces.reshape(source_trace.shape), coef.transpose(0, 2, 1)

    where = P(("wl", "sy"), "sx", None, None, None, None)
    return jax.shard_map(
        per_device,
        mesh=mesh,
        in_specs=(P(("wl", "sy"), "sx", None, None, None), where, where, where, P("wl", None, None)),
        out_specs=(where, P("wl", None, None)),
        check_vma=False,
    )
```

```python
import functools

import jax
import jax.numpy as jnp
from jax import lax
from jax.experimental import pallas as pl
from jax.experimental.pallas import tpu as pltpu
from jax.sharding import PartitionSpec as P

ITERS = 6
LANES = 128
MESH = pl.DeviceIdType.MESH
HIGH = lax.Precision.HIGHEST
NORTH, SOUTH, WEST, EAST = 0, 1, 2, 3
OUT_OF = {NORTH: SOUTH, SOUTH: NORTH, WEST: EAST, EAST: WEST}


def dot(a, b, contract, precision=None):
    return lax.dot_general(
        a, b, (contract, ((), ())), preferred_element_type=jnp.float32, precision=precision
    )


def turned(pair, half):
    return jnp.concatenate([-pair[:, half:], pair[:, :half]], axis=1)


def kernel(
    dims,
    map_hbm,
    src_hbm,
    res_hbm,
    pro_hbm,
    inv_ref,
    out_hbm,
    coef_ref,
    raw,
    src_raw,
    res_raw,
    pro_raw,
    src_ref,
    table,
    lhs,
    acc,
    src_hi,
    src_lo,
    out_hi,
    out_lo,
    sent,
    got,
    lift,
    res_split,
    corner_table,
    corner_acc,
    corner_src,
    corner_out,
    corner_in,
    part,
    plane_in,
    line_out,
    line_in,
    col_out,
    col_in,
    fix,
    last_sum,
    map_sem,
    load_sem,
    send_sem,
    recv_sem,
    wsend_sem,
    wrecv_sem,
    csend_sem,
    crecv_sem,
    asend_sem,
    arecv_sem,
):
    ny, nx, nz, s2, q2, thirds = dims
    cells = thirds * LANES
    nsy = ny * nx
    rows_all = s2 + q2
    half_s, half_q = s2 // 2, q2 // 2
    sy, sx = lax.axis_index("sy"), lax.axis_index("sx")
    wl = lax.axis_index("wl")
    yy = sy // nx

    def dev(row, col):
        return (row, col, wl)

    def place(side, t):
        return (order.index(t) * 4 + side) * LANES

    up, down = lax.rem(sy + nsy - 1, nsy), lax.rem(sy + 1, nsy)
    left, right = lax.rem(sx + nz - 1, nz), lax.rem(sx + 1, nz)
    peer = {NORTH: dev(up, sx), SOUTH: dev(down, sx), WEST: dev(sy, left), EAST: dev(sy, right)}
    diag = (dev(up, left), dev(up, right), dev(down, left), dev(down, right))
    has = {NORTH: sy > 0, SOUTH: sy < nsy - 1, WEST: sx > 0, EAST: sx < nz - 1}
    has_diag = (
        (sy > 0) & (sx > 0),
        (sy > 0) & (sx < nz - 1),
        (sy < nsy - 1) & (sx > 0),
        (sy < nsy - 1) & (sx < nz - 1),
    )

    depth = 4 * cells
    order = (0, *range(2, thirds), 1)
    early = 4 * LANES * (thirds - 1)
    blocks = depth // LANES
    flat_map = map_hbm.reshape(2 * depth, depth)
    loads = [
        pltpu.make_async_copy(
            flat_map.at[pl.ds(2 * LANES * b, 2 * LANES)],
            raw.at[pl.ds(2 * LANES * b, 2 * LANES)],
            map_sem.at[b],
        )
        for b in range(blocks)
    ]
    flat_src = src_hbm.reshape(4 * s2, cells)
    flat_pro = pro_hbm.reshape(4 * q2, cells)
    flat_res = res_hbm.reshape(4 * q2, cells)

    def third(flat, held, which):
        return [
            pltpu.make_async_copy(
                flat.at[:, pl.ds(t * LANES, LANES)], held.at[t], load_sem.at[which, t]
            )
            for t in range(thirds)
        ]

    src_load = third(flat_src, src_raw, 0)
    pro_load = third(flat_pro, pro_raw, 1)
    res_load = third(flat_res, res_raw, 2)
    for copy in (*src_load, *pro_load, *res_load):
        copy.start()
    for b in range(blocks):
        loads[b].start()

    barrier = pltpu.get_barrier_semaphore()
    met = 0
    for target in (*peer.values(), *diag):
        pl.semaphore_signal(barrier, inc=1, device_id=target, device_id_type=MESH)
        met += 1
    for d in range(1, nsy):
        target = dev(lax.rem(sy + d, nsy), sx)
        pl.semaphore_signal(barrier, inc=1, device_id=target, device_id_type=MESH)
        met += 1
    for d in range(1, nz):
        target = dev(sy, lax.rem(sx + d, nz))
        pl.semaphore_signal(barrier, inc=1, device_id=target, device_id_type=MESH)
        met += 1
    for t in order:
        src_load[t].wait()
        res_load[t].wait()
        for side in range(4):
            at = place(side, t)
            value = src_raw[t, pl.ds(side, s2, stride=4), :]
            src_ref[side, t] = value
            sent[1, side, t, 0:s2] = value
            sent[1, side, t, s2:] = res_raw[t, pl.ds(side, q2, stride=4), :]
    pl.semaphore_wait(barrier, met)

    lane = lax.broadcasted_iota(jnp.int32, (1, LANES), 1)

    def rows_of(e):
        return rows_all if e in (2, 3) else s2

    def side_copy(e, side, t):
        par, rows = e % 2, rows_of(e)
        return pltpu.make_async_remote_copy(
            src_ref=sent.at[par, side, t, pl.ds(0, rows)],
            dst_ref=got.at[par, OUT_OF[side], t, pl.ds(0, rows)],
            send_sem=send_sem.at[par, side, t],
            recv_sem=recv_sem.at[par, OUT_OF[side], t],
            device_id=peer[side],
            device_id_type=MESH,
        )

    def weight_copy(side, t):
        return pltpu.make_async_remote_copy(
            src_ref=sent.at[1, side, t, pl.ds(s2, q2)],
            dst_ref=got.at[1, OUT_OF[side], t, pl.ds(s2, q2)],
            send_sem=wsend_sem.at[side, t],
            recv_sem=wrecv_sem.at[OUT_OF[side], t],
            device_id=peer[side],
            device_id_type=MESH,
        )

    def corner_copy(e, k):
        par = e % 2
        return pltpu.make_async_remote_copy(
            src_ref=corner_out.at[par],
            dst_ref=corner_in.at[par, 3 - k],
            send_sem=csend_sem.at[par, k],
            recv_sem=crecv_sem.at[par, 3 - k],
            device_id=diag[k],
            device_id_type=MESH,
        )

    def source_corners(block):
        last = thirds - 1
        n0, n1 = block(NORTH, 0)[:, 0:1], block(NORTH, last)[:, LANES - 1 :]
        s0, s1 = block(SOUTH, 0)[:, 0:1], block(SOUTH, last)[:, LANES - 1 :]
        w0, w1 = block(WEST, 0)[:, 0:1], block(WEST, last)[:, LANES - 1 :]
        e0, e1 = block(EAST, 0)[:, 0:1], block(EAST, last)[:, LANES - 1 :]
        nw, ne, sw, se = n0 + w0, n1 + e0, s0 + w1, s1 + e1
        return jnp.where(
            lane == 0, nw, jnp.where(lane == 1, ne, jnp.where(lane == 2, sw, se))
        )

    def send_corners(e, z):
        first = z[0:LANES].T[0:4]
        if z.shape[0] > s2:
            spare = jnp.zeros((2 * LANES - z.shape[0], LANES), jnp.float32)
            second = jnp.concatenate([z[LANES:], spare], axis=0).T[0:4]
        else:
            second = jnp.zeros_like(first)
        corner_out[e % 2] = jnp.concatenate([first, second], axis=0)
        for k in range(4):
            corner_copy(e, k).start()

    chunk = part.shape[2]

    def stage_a(a, j):
        d = j
        target = lax.rem(sy + d, nsy)
        return pltpu.make_async_remote_copy(
            src_ref=part.at[a, target // nx],
            dst_ref=plane_in.at[a, nsy - d],
            send_sem=asend_sem.at[a, 0],
            recv_sem=arecv_sem.at[a, 0],
            device_id=dev(target, sx),
            device_id_type=MESH,
        )

    def stage_b(a, d):
        return pltpu.make_async_remote_copy(
            src_ref=line_out.at[a],
            dst_ref=line_in.at[a, nz - d],
            send_sem=asend_sem.at[a, 1],
            recv_sem=arecv_sem.at[a, 1],
            device_id=dev(sy, lax.rem(sx + d, nz)),
            device_id_type=MESH,
        )

    def stage_c(a, d):
        return pltpu.make_async_remote_copy(
            src_ref=col_out.at[a],
            dst_ref=col_in.at[a, ny - d],
            send_sem=asend_sem.at[a, 2],
            recv_sem=arecv_sem.at[a, 2],
            device_id=dev(lax.rem(sy + d * nx, nsy), sx),
            device_id_type=MESH,
        )

    def whole(a, stage):
        buf = (plane_in, line_in, col_in)[stage]
        n = (nsy, nz, ny)[stage]
        ref = buf.at[a, pl.ds(1, n - 1)]
        return pltpu.make_async_remote_copy(
            src_ref=ref,
            dst_ref=ref,
            send_sem=asend_sem.at[a, stage],
            recv_sem=arecv_sem.at[a, stage],
            device_id=peer[EAST],
            device_id_type=MESH,
        )

    def summed(values):
        while len(values) > 1:
            values = [
                values[i] + values[i + 1] if i + 1 < len(values) else values[i]
                for i in range(0, len(values), 2)
            ]
        return values[0]

    def start_sum(a, payload):
        for j in range(ny):
            part[a, j] = payload[j * chunk : (j + 1) * chunk]
        for d in range(1, nsy):
            stage_a(a, d).start()

    def sum_b(a):
        whole(a, 0).wait_recv()
        plane_in[a, 0] = part[a, yy]
        line_out[a] = summed([plane_in[a, lax.rem(j - sy + nsy, nsy)] for j in range(nsy)])
        for d in range(1, nz):
            stage_b(a, d).start()

    def sum_c(a):
        whole(a, 1).wait_recv()
        line_in[a, 0] = line_out[a]
        col_out[a] = summed([line_in[a, lax.rem(j - sx + nz, nz)] for j in range(nz)])
        for d in range(1, ny):
            stage_c(a, d).start()

    def sum_end(a):
        whole(a, 2).wait_recv()
        col_in[a, 0] = col_out[a]
        return jnp.concatenate([col_in[a, lax.rem(j - yy + ny, ny)] for j in range(ny)], axis=0)

    corners = source_corners(lambda side, t: sent[1, side, t])
    corner_src[...] = corners[0:s2]
    send_corners(1, corners)
    for t in order:
        for side in range(4):
            side_copy(1, side, t).start()
    for t in order:
        for side in range(4):
            weight_copy(side, t).start()

    def split(value, side, t, first, last):
        at = place(side, t)
        hi = value.astype(jnp.bfloat16)
        out_hi[first:last, at : at + LANES] = hi
        out_lo[first:last, at : at + LANES] = (value - hi.astype(jnp.float32)).astype(jnp.bfloat16)

    for t in order:
        for side in range(4):
            at, value = place(side, t), src_ref[side, t]
            hi = value.astype(jnp.bfloat16)
            src_hi[:, at : at + LANES] = hi
            src_lo[:, at : at + LANES] = (value - hi.astype(jnp.float32)).astype(jnp.bfloat16)

    for t in order:
        pro_load[t].wait()
        for side in range(4):
            at = place(side, t)
            lhs[s2:rows_all, at : at + LANES] = pro_raw[t, pl.ds(side, q2, stride=4), :].astype(
                jnp.bfloat16
            )

    rows_i = lax.broadcasted_iota(jnp.int32, (2 * LANES, 2 * LANES), 0)
    cols_i = lax.broadcasted_iota(jnp.int32, (2 * LANES, 2 * LANES), 1)
    wanted = jnp.where(rows_i < LANES, 2 * rows_i, 2 * (rows_i - LANES) + 1)
    chosen = jnp.where(cols_i == wanted, 1.0, 0.0).astype(jnp.bfloat16)
    corner_ends = (
        ((NORTH, 0), (WEST, 0)),
        ((NORTH, 1), (EAST, 0)),
        ((SOUTH, 0), (WEST, 1)),
        ((SOUTH, 1), (EAST, 1)),
    )
    for b in range(blocks):
        loads[b].wait()
        exact = dot(chosen, raw[2 * LANES * b : 2 * LANES * (b + 1)], ((1,), (0,)))
        row = place(b // thirds, b % thirds)
        picked = jnp.zeros((LANES, LANES), jnp.float32)
        for c in (0, 1):
            for j in (0, 1):
                for k in range(4):
                    side, end = corner_ends[k][j]
                    at = side * cells + end * (thirds - 1) * LANES
                    goal = c * 8 + j * 4 + k
                    moved = pltpu.roll(
                        exact[c * LANES : (c + 1) * LANES, at : at + LANES], (goal + end) % LANES, 1
                    )
                    picked = jnp.where(lane == goal, moved, picked)
        corner_table[row : row + LANES] = picked.astype(jnp.bfloat16)
        parted = exact.astype(jnp.bfloat16)
        for side in range(4):
            h, k = side // 2, 2 * (side % 2) * LANES
            for t in range(thirds):
                at = side * cells + t * LANES
                for c in (0, 1):
                    table[t, h, row : row + LANES, k + c * LANES : k + (c + 1) * LANES] = parted[
                        c * LANES : (c + 1) * LANES, at : at + LANES
                    ]

    def restrict(first, last):
        return restricted(out_hi[first:last], out_lo[first:last])

    def restricted(hi, lo):
        half = hi.shape[0] // 2
        both = dot(res_split[...], hi, ((1,), (1,)))
        rest = dot(res_split[0:q2], lo, ((1,), (1,)))
        u = both[0:q2] + both[q2:] + rest
        return u[0:half_q] + turned(u[half_q:], half)

    def coarse(total):
        stacked = jnp.concatenate([total, turned(total, half_s)], axis=0)
        coef = dot(inv_ref[...], stacked, ((0,), (0,)), HIGH)
        return coef

    def stack_of(coef):
        return jnp.concatenate([coef, turned(coef, half_s)], axis=0)

    def lifted(coef, k, first=0, last=depth):
        stack = stack_of(coef)
        hi = stack.astype(jnp.bfloat16)
        rest = (stack - hi.astype(jnp.float32)).astype(jnp.bfloat16)
        three = jnp.concatenate([hi, hi, rest], axis=0)
        fix[:, first:last] = dot(three, lift[k, :, first:last], ((0,), (0,)))

    def corner_columns(e):
        par, rows = e % 2, rows_of(e)
        for k in range(4):
            corner_copy(e, k).wait_recv()
        tile = []
        for base in (0, 4) if e <= 3 else (0,):
            for k in range(4):
                row = corner_in[par, k, base + 3 - k : base + 4 - k]
                tile.append(jnp.where(has_diag[k], 0.5 * row, 0.0))
        spare = jnp.zeros((LANES - len(tile), LANES), jnp.float32)
        flat = jnp.concatenate([*tile, spare], axis=0).T
        cols = flat[:, 0:4]
        if e <= 3:
            cols = jnp.concatenate([cols, flat[0:q2, 4:8]], axis=0)
        nw, ne, sw, se = (cols[:, k : k + 1] for k in range(4))
        return {NORTH: (nw, ne), SOUTH: (sw, se), WEST: (nw, sw), EAST: (ne, se)}

    def arrived(par, ends, side, t, first, last):
        value = jnp.where(has[side], got[par, side, t, first:last], 0.0)
        if t == 0:
            value += jnp.where(lane == 0, ends[side][0][first:last], 0.0)
        if t == thirds - 1:
            value += jnp.where(lane == LANES - 1, ends[side][1][first:last], 0.0)
        return value

    def receive_weights(ends):
        for t in order:
            for side in range(4):
                weight_copy(OUT_OF[side], t).wait_recv()
                at = place(side, t)
                extra = arrived(1, ends, side, t, s2, rows_all)
                hi = extra.astype(jnp.bfloat16)
                res_split[0:q2, at : at + LANES] = hi
                res_split[q2:, at : at + LANES] = (extra - hi.astype(jnp.float32)).astype(
                    jnp.bfloat16
                )
        for t in order:
            for side in range(4):
                weight_copy(side, t).wait_send()

    def receive(e, some, fixed, ends=None):
        par, rows = e % 2, rows_of(e)
        first, last = place(0, some[0]), place(0, some[-1]) + 4 * LANES
        ends = corner_columns(e) if ends is None else ends

        def incoming(side, t, first, last):
            return arrived(par, ends, side, t, first, last)

        for t in some:
            for side in range(4):
                side_copy(e, OUT_OF[side], t).wait_recv()
                if rows > s2:
                    at = place(side, t)
                    extra = incoming(side, t, s2, rows)
                    hi = extra.astype(jnp.bfloat16)
                    rest = (extra - hi.astype(jnp.float32)).astype(jnp.bfloat16)
                    lift[e - 2, 0:q2, at : at + LANES] = hi
                    lift[e - 2, q2 : 2 * q2, at : at + LANES] = rest
                    lift[e - 2, 2 * q2 :, at : at + LANES] = hi
                    if e == 2:
                        lhs[s2:, at : at + LANES] = hi
        if e == 3:
            lifted(fixed, 1, first, last)
        for t in some:
            for side in range(4):
                at = place(side, t)
                top = incoming(side, t, 0, s2)
                if fixed is not None:
                    top += fix[:, at : at + LANES]
                if e == ITERS:
                    last_sum[:, at : at + LANES] = top
                else:
                    lhs[0:s2, at : at + LANES] = top.astype(jnp.bfloat16)
        return ends

    def sends_done(e):
        for t in order:
            for side in range(4):
                side_copy(e, side, t).wait_send()
        for k in range(4):
            corner_copy(e, k).wait_send()

    def multiply_early(e):
        rows = rows_of(e)
        corner_acc[0:rows] = dot(lhs[0:rows, 0:early], corner_table[0:early], ((1,), (0,)))
        for t in order:
            for h in (0, 1):
                acc[t, h, 0:rows] = dot(lhs[0:rows, 0:early], table[t, h, 0:early], ((1,), (0,)))

    def multiply_late(e):
        rows, par = rows_of(e), e % 2
        if e >= 3:
            sends_done(e - 2)

        z = corner_acc[0:rows] + dot(lhs[0:rows, early:], corner_table[early:], ((1,), (0,)))
        re = z + pltpu.roll(z, LANES - 4, 1)
        im = pltpu.roll(re, LANES - 8, 1)
        a, b = half_s, s2
        parts = [
            re[0:a] - im[a:b] + corner_src[0:a],
            im[0:a] + re[a:b] + corner_src[a:b],
        ]
        if rows > s2:
            a, b = s2 + half_q, s2 + q2
            parts += [re[s2:a] - im[a:b], im[s2:a] + re[a:b]]
        send_corners(e, jnp.concatenate(parts, axis=0))

        for t in order:
            for h in (0, 1):
                product = acc[t, h, 0:rows] + dot(
                    lhs[0:rows, early:], table[t, h, early:], ((1,), (0,))
                )
                for k in (0, 1):
                    side = 2 * h + k
                    re = product[:, 2 * k * LANES : (2 * k + 1) * LANES]
                    im = product[:, (2 * k + 1) * LANES : (2 * k + 2) * LANES]
                    a, b = half_s, s2
                    out_re = re[0:a] - im[a:b] + src_ref[side, t, 0:a]
                    out_im = im[0:a] + re[a:b] + src_ref[side, t, a:b]
                    sent[par, side, t, 0:a] = out_re
                    sent[par, side, t, a:b] = out_im
                    if e < ITERS:
                        split(out_re, side, t, 0, a)
                        split(out_im, side, t, a, b)
                    if rows > s2:
                        a, b = s2 + half_q, s2 + q2
                        out_re = re[s2:a] - im[a:b]
                        out_im = im[s2:a] + re[a:b]
                        sent[par, side, t, s2:a] = out_re
                        sent[par, side, t, a:b] = out_im
                        split(out_re, side, t, s2, a)
                        split(out_im, side, t, a, b)
                    side_copy(e, side, t).start()

    coef, share = {}, {}

    def finish(j):
        total = sum_end(j)
        if j == 2:
            share[0] = sum_end(0)[:, 0:q2]
        if j == 3:
            share[1] = sum_end(ITERS)[:, 0:q2]
        for k in (0, 1):
            if j - 1 - k >= 1:
                total += dot(share[k], stack_of(coef[j - 1 - k]), ((1,), (0,)), HIGH)
        coef[j] = coarse(total)

    def lifted_rows():
        half = restrict(s2, rows_all)
        return jnp.concatenate([half, jnp.zeros((half_q, LANES - q2), jnp.float32)], axis=1)

    for i in range(1, ITERS):
        ends = receive(i, order[:-1], coef.get(i - 2))
        multiply_early(i + 1)
        if i >= 2:
            sum_b(i)
        if i == 2:
            sum_b(0)
        if i == 3:
            sum_b(ITERS)
        receive(i, order[-1:], coef.get(i - 2), ends)
        if i == 1:
            receive_weights(ends)
            start_sum(1, restricted(src_hi[...], src_lo[...]))
        multiply_late(i + 1)
        if i == 2:
            sum_c(1)
        if i < ITERS - 1:
            start_sum(i + 1, restrict(0, s2))
        if i == 1:
            start_sum(0, lifted_rows())
            sum_b(1)
        if i == 2:
            start_sum(ITERS, lifted_rows())
        if i >= 3:
            finish(i - 1)
            lifted(coef[i - 1], 1)
        if i >= 2:
            sum_c(i)
        if i == 2:
            sum_c(0)
            finish(1)
        if i == 3:
            sum_c(ITERS)

    ends = receive(ITERS, order[:-1], coef[ITERS - 2])
    receive(ITERS, order[-1:], coef[ITERS - 2], ends)
    finish(ITERS - 1)
    lifted(coef[ITERS - 1], 0)
    flat_out = out_hbm.reshape(4 * s2, cells)
    stores = [
        pltpu.make_async_copy(
            src_raw.at[t], flat_out.at[:, pl.ds(t * LANES, LANES)], load_sem.at[0, t]
        )
        for t in range(thirds)
    ]
    for t in range(thirds):
        for side in range(4):
            at = place(side, t)
            src_raw[t, pl.ds(side, s2, stride=4), :] = (
                last_sum[:, at : at + LANES] + fix[:, at : at + LANES]
            )
        stores[t].start()
    coef_ref[0] = coef[ITERS - 1][:, 0:half_s]
    coef_ref[1] = coef[ITERS - 1][:, half_s:]
    sends_done(ITERS - 1)
    sends_done(ITERS)
    for a in range(ITERS + 1):
        for stage in range(3):
            whole(a, stage).wait_send()
    for t in range(thirds):
        stores[t].wait()


def solution(mesh):
    nsy, nz = mesh.shape["sy"], mesh.shape["sx"]
    nx = 4
    ny = nsy // nx

    def per_device(interface_map, source_trace, restriction, prolongation, coarse_inverse):
        src_count, cells = source_trace.shape[3], source_trace.shape[5]
        width = restriction.shape[3]
        thirds = cells // LANES
        s2, q2 = 2 * src_count, 2 * width
        rows = s2 + q2
        depth = 4 * cells
        dims = (ny, nx, nz, s2, q2, thirds)
        chunk = width // ny
        vmem = pl.BlockSpec(memory_space=pltpu.VMEM)
        hbm = pl.BlockSpec(memory_space=pl.ANY)
        traces, coef = pl.pallas_call(
            functools.partial(kernel, dims),
            out_shape=(
                jax.ShapeDtypeStruct((2, src_count, 4, cells), jnp.float32),
                jax.ShapeDtypeStruct((2, width, src_count), jnp.float32),
            ),
            in_specs=[hbm, hbm, hbm, hbm, vmem],
            out_specs=(hbm, vmem),
            scratch_shapes=[
                pltpu.VMEM((2 * depth, depth), jnp.bfloat16),
                pltpu.VMEM((thirds, 4 * s2, LANES), jnp.float32),
                pltpu.VMEM((thirds, 4 * q2, LANES), jnp.float32),
                pltpu.VMEM((thirds, 4 * q2, LANES), jnp.float32),
                pltpu.VMEM((4, thirds, s2, LANES), jnp.float32),
                pltpu.VMEM((thirds, 2, depth, 4 * LANES), jnp.bfloat16),
                pltpu.VMEM((rows, depth), jnp.bfloat16),
                pltpu.VMEM((thirds, 2, rows, 4 * LANES), jnp.float32),
                pltpu.VMEM((s2, depth), jnp.bfloat16),
                pltpu.VMEM((s2, depth), jnp.bfloat16),
                pltpu.VMEM((rows, depth), jnp.bfloat16),
                pltpu.VMEM((rows, depth), jnp.bfloat16),
                pltpu.VMEM((2, 4, thirds, rows, LANES), jnp.float32),
                pltpu.VMEM((2, 4, thirds, rows, LANES), jnp.float32),
                pltpu.VMEM((2, 3 * q2, depth), jnp.bfloat16),
                pltpu.VMEM((2 * q2, depth), jnp.bfloat16),
                pltpu.VMEM((depth, LANES), jnp.bfloat16),
                pltpu.VMEM((rows, LANES), jnp.float32),
                pltpu.VMEM((s2, LANES), jnp.float32),
                pltpu.VMEM((2, 8, LANES), jnp.float32),
                pltpu.VMEM((2, 4, 8, LANES), jnp.float32),
                pltpu.VMEM((ITERS + 1, ny, chunk, LANES), jnp.float32),
                pltpu.VMEM((ITERS + 1, nsy, chunk, LANES), jnp.float32),
                pltpu.VMEM((ITERS + 1, chunk, LANES), jnp.float32),
                pltpu.VMEM((ITERS + 1, nz, chunk, LANES), jnp.float32),
                pltpu.VMEM((ITERS + 1, chunk, LANES), jnp.float32),
                pltpu.VMEM((ITERS + 1, ny, chunk, LANES), jnp.float32),
                pltpu.VMEM((s2, depth), jnp.float32),
                pltpu.VMEM((s2, depth), jnp.float32),
                pltpu.SemaphoreType.DMA((depth // LANES,)),
                pltpu.SemaphoreType.DMA((3, thirds)),
                pltpu.SemaphoreType.DMA((2, 4, thirds)),
                pltpu.SemaphoreType.DMA((2, 4, thirds)),
                pltpu.SemaphoreType.DMA((4, thirds)),
                pltpu.SemaphoreType.DMA((4, thirds)),
                pltpu.SemaphoreType.DMA((2, 4)),
                pltpu.SemaphoreType.DMA((2, 4)),
                pltpu.SemaphoreType.DMA((ITERS + 1, 3)),
                pltpu.SemaphoreType.DMA((ITERS + 1, 3)),
            ],
            compiler_params=pltpu.CompilerParams(
                collective_id=0, has_side_effects=True, vmem_limit_bytes=60 * 1024 * 1024
            ),
        )(
            interface_map.reshape(depth, 2, depth),
            source_trace.reshape(2, src_count, 4, cells),
            restriction.reshape(2, width, 4, cells),
            prolongation.reshape(2, width, 4, cells),
            coarse_inverse.reshape(q2, width),
        )
        return traces.reshape(source_trace.shape), coef.transpose(0, 2, 1)

    where = P(("wl", "sy"), "sx", None, None, None, None)
    return jax.shard_map(
        per_device,
        mesh=mesh,
        in_specs=(P(("wl", "sy"), "sx", None, None, None), where, where, where, P("wl", None, None)),
        out_specs=(where, P("wl", None, None)),
        check_vma=False,
    )
```

```python
import functools

import jax
import jax.numpy as jnp
from jax import lax
from jax.experimental import pallas as pl
from jax.experimental.pallas import tpu as pltpu
from jax.sharding import PartitionSpec as P

ITERS = 6
LANES = 128
MESH = pl.DeviceIdType.MESH
HIGH = lax.Precision.HIGHEST
NORTH, SOUTH, WEST, EAST = 0, 1, 2, 3
OUT_OF = {NORTH: SOUTH, SOUTH: NORTH, WEST: EAST, EAST: WEST}


def dot(a, b, contract, precision=None):
    return lax.dot_general(
        a, b, (contract, ((), ())), preferred_element_type=jnp.float32, precision=precision
    )


def turned(pair, half):
    return jnp.concatenate([-pair[:, half:], pair[:, :half]], axis=1)


def kernel(
    dims,
    map_hbm,
    src_hbm,
    res_hbm,
    pro_hbm,
    inv_hbm,
    out_hbm,
    coef_hbm,
    inv_ref,
    coef_ref,
    raw,
    src_raw,
    res_raw,
    pro_raw,
    src_ref,
    table,
    lhs,
    acc,
    src_hi,
    src_lo,
    out_hi,
    out_lo,
    sent,
    got,
    lift,
    res_split,
    corner_table,
    corner_acc,
    corner_src,
    corner_out,
    corner_in,
    part,
    plane_in,
    line_out,
    line_in,
    col_out,
    col_in,
    fix,
    last_sum,
    map_sem,
    load_sem,
    small_sem,
    send_sem,
    recv_sem,
    wsend_sem,
    wrecv_sem,
    csend_sem,
    crecv_sem,
    asend_sem,
    arecv_sem,
):
    ny, nx, nz, s2, q2, thirds = dims
    cells = thirds * LANES
    nsy = ny * nx
    rows_all = s2 + q2
    half_s, half_q = s2 // 2, q2 // 2
    sy, sx = lax.axis_index("sy"), lax.axis_index("sx")
    wl = lax.axis_index("wl")
    yy = sy // nx

    def dev(row, col):
        return (row, col, wl)

    def place(side, t):
        return (order.index(t) * 4 + side) * LANES

    up, down = lax.rem(sy + nsy - 1, nsy), lax.rem(sy + 1, nsy)
    left, right = lax.rem(sx + nz - 1, nz), lax.rem(sx + 1, nz)
    peer = {NORTH: dev(up, sx), SOUTH: dev(down, sx), WEST: dev(sy, left), EAST: dev(sy, right)}
    diag = (dev(up, left), dev(up, right), dev(down, left), dev(down, right))
    has = {NORTH: sy > 0, SOUTH: sy < nsy - 1, WEST: sx > 0, EAST: sx < nz - 1}
    has_diag = (
        (sy > 0) & (sx > 0),
        (sy > 0) & (sx < nz - 1),
        (sy < nsy - 1) & (sx > 0),
        (sy < nsy - 1) & (sx < nz - 1),
    )

    depth = 4 * cells
    order = (0, *range(2, thirds), 1)
    early = 4 * LANES * (thirds - 1)
    blocks = depth // LANES
    flat_map = map_hbm.reshape(2 * depth, depth)
    loads = [
        pltpu.make_async_copy(
            flat_map.at[pl.ds(2 * LANES * b, 2 * LANES)],
            raw.at[pl.ds(2 * LANES * b, 2 * LANES)],
            map_sem.at[b],
        )
        for b in range(blocks)
    ]
    flat_src = src_hbm.reshape(4 * s2, cells)
    flat_pro = pro_hbm.reshape(4 * q2, cells)
    flat_res = res_hbm.reshape(4 * q2, cells)

    def third(flat, held, which):
        return [
            pltpu.make_async_copy(
                flat.at[:, pl.ds(t * LANES, LANES)], held.at[t], load_sem.at[which, t]
            )
            for t in range(thirds)
        ]

    src_load = third(flat_src, src_raw, 0)
    pro_load = third(flat_pro, pro_raw, 1)
    res_load = third(flat_res, res_raw, 2)
    inv_load = pltpu.make_async_copy(inv_hbm, inv_ref, small_sem.at[0])
    coef_store = pltpu.make_async_copy(coef_ref, coef_hbm, small_sem.at[1])
    for copy in (*src_load, *res_load, *pro_load, inv_load):
        copy.start()
    for b in range(blocks):
        loads[b].start()

    barrier = pltpu.get_barrier_semaphore()
    met = 0
    for target in (*peer.values(), *diag):
        pl.semaphore_signal(barrier, inc=1, device_id=target, device_id_type=MESH)
        met += 1
    for d in range(1, nsy):
        target = dev(lax.rem(sy + d, nsy), sx)
        pl.semaphore_signal(barrier, inc=1, device_id=target, device_id_type=MESH)
        met += 1
    for d in range(1, nz):
        target = dev(sy, lax.rem(sx + d, nz))
        pl.semaphore_signal(barrier, inc=1, device_id=target, device_id_type=MESH)
        met += 1
    for t in order:
        src_load[t].wait()
        res_load[t].wait()
        for side in range(4):
            at = place(side, t)
            value = src_raw[t, pl.ds(side, s2, stride=4), :]
            src_ref[side, t] = value
            sent[1, side, t, 0:s2] = value
            sent[1, side, t, s2:] = res_raw[t, pl.ds(side, q2, stride=4), :]
    pl.semaphore_wait(barrier, met)

    lane = lax.broadcasted_iota(jnp.int32, (1, LANES), 1)

    def rows_of(e):
        return rows_all if e in (2, 3) else s2

    def side_copy(e, side, t):
        par, rows = e % 2, rows_of(e)
        return pltpu.make_async_remote_copy(
            src_ref=sent.at[par, side, t, pl.ds(0, rows)],
            dst_ref=got.at[par, OUT_OF[side], t, pl.ds(0, rows)],
            send_sem=send_sem.at[par, side, t],
            recv_sem=recv_sem.at[par, OUT_OF[side], t],
            device_id=peer[side],
            device_id_type=MESH,
        )

    def weight_copy(side, t):
        return pltpu.make_async_remote_copy(
            src_ref=sent.at[1, side, t, pl.ds(s2, q2)],
            dst_ref=got.at[1, OUT_OF[side], t, pl.ds(s2, q2)],
            send_sem=wsend_sem.at[side, t],
            recv_sem=wrecv_sem.at[OUT_OF[side], t],
            device_id=peer[side],
            device_id_type=MESH,
        )

    def corner_copy(e, k):
        par = e % 2
        return pltpu.make_async_remote_copy(
            src_ref=corner_out.at[par],
            dst_ref=corner_in.at[par, 3 - k],
            send_sem=csend_sem.at[par, k],
            recv_sem=crecv_sem.at[par, 3 - k],
            device_id=diag[k],
            device_id_type=MESH,
        )

    def source_corners(block):
        last = thirds - 1
        n0, n1 = block(NORTH, 0)[:, 0:1], block(NORTH, last)[:, LANES - 1 :]
        s0, s1 = block(SOUTH, 0)[:, 0:1], block(SOUTH, last)[:, LANES - 1 :]
        w0, w1 = block(WEST, 0)[:, 0:1], block(WEST, last)[:, LANES - 1 :]
        e0, e1 = block(EAST, 0)[:, 0:1], block(EAST, last)[:, LANES - 1 :]
        nw, ne, sw, se = n0 + w0, n1 + e0, s0 + w1, s1 + e1
        return jnp.where(
            lane == 0, nw, jnp.where(lane == 1, ne, jnp.where(lane == 2, sw, se))
        )

    def send_corners(e, z):
        first = z[0:LANES].T[0:4]
        if z.shape[0] > s2:
            spare = jnp.zeros((2 * LANES - z.shape[0], LANES), jnp.float32)
            second = jnp.concatenate([z[LANES:], spare], axis=0).T[0:4]
        else:
            second = jnp.zeros_like(first)
        corner_out[e % 2] = jnp.concatenate([first, second], axis=0)
        for k in range(4):
            corner_copy(e, k).start()

    chunk = part.shape[2]

    def stage_a(a, j):
        d = j
        target = lax.rem(sy + d, nsy)
        return pltpu.make_async_remote_copy(
            src_ref=part.at[a, target // nx],
            dst_ref=plane_in.at[a, nsy - d],
            send_sem=asend_sem.at[a, 0],
            recv_sem=arecv_sem.at[a, 0],
            device_id=dev(target, sx),
            device_id_type=MESH,
        )

    def stage_b(a, d):
        return pltpu.make_async_remote_copy(
            src_ref=line_out.at[a],
            dst_ref=line_in.at[a, nz - d],
            send_sem=asend_sem.at[a, 1],
            recv_sem=arecv_sem.at[a, 1],
            device_id=dev(sy, lax.rem(sx + d, nz)),
            device_id_type=MESH,
        )

    def stage_c(a, d):
        return pltpu.make_async_remote_copy(
            src_ref=col_out.at[a],
            dst_ref=col_in.at[a, ny - d],
            send_sem=asend_sem.at[a, 2],
            recv_sem=arecv_sem.at[a, 2],
            device_id=dev(lax.rem(sy + d * nx, nsy), sx),
            device_id_type=MESH,
        )

    def whole(a, stage):
        buf = (plane_in, line_in, col_in)[stage]
        n = (nsy, nz, ny)[stage]
        ref = buf.at[a, pl.ds(1, n - 1)]
        return pltpu.make_async_remote_copy(
            src_ref=ref,
            dst_ref=ref,
            send_sem=asend_sem.at[a, stage],
            recv_sem=arecv_sem.at[a, stage],
            device_id=peer[EAST],
            device_id_type=MESH,
        )

    def summed(values):
        while len(values) > 1:
            values = [
                values[i] + values[i + 1] if i + 1 < len(values) else values[i]
                for i in range(0, len(values), 2)
            ]
        return values[0]

    def start_sum(a, payload):
        for j in range(ny):
            part[a, j] = payload[j * chunk : (j + 1) * chunk]
        for d in range(1, nsy):
            stage_a(a, d).start()

    def sum_b(a):
        whole(a, 0).wait_recv()
        plane_in[a, 0] = part[a, yy]
        line_out[a] = summed([plane_in[a, lax.rem(j - sy + nsy, nsy)] for j in range(nsy)])
        for d in range(1, nz):
            stage_b(a, d).start()

    def sum_c(a):
        whole(a, 1).wait_recv()
        line_in[a, 0] = line_out[a]
        col_out[a] = summed([line_in[a, lax.rem(j - sx + nz, nz)] for j in range(nz)])
        for d in range(1, ny):
            stage_c(a, d).start()

    def sum_end(a):
        whole(a, 2).wait_recv()
        col_in[a, 0] = col_out[a]
        return jnp.concatenate([col_in[a, lax.rem(j - yy + ny, ny)] for j in range(ny)], axis=0)

    corners = source_corners(lambda side, t: sent[1, side, t])
    corner_src[...] = corners[0:s2]
    send_corners(1, corners)
    for t in order:
        for side in range(4):
            side_copy(1, side, t).start()
    for t in order:
        for side in range(4):
            weight_copy(side, t).start()

    def split(value, side, t, first, last):
        at = place(side, t)
        hi = value.astype(jnp.bfloat16)
        out_hi[first:last, at : at + LANES] = hi
        out_lo[first:last, at : at + LANES] = (value - hi.astype(jnp.float32)).astype(jnp.bfloat16)

    for t in order:
        for side in range(4):
            at, value = place(side, t), src_ref[side, t]
            hi = value.astype(jnp.bfloat16)
            src_hi[:, at : at + LANES] = hi
            src_lo[:, at : at + LANES] = (value - hi.astype(jnp.float32)).astype(jnp.bfloat16)

    inv_load.wait()
    for t in order:
        pro_load[t].wait()
        for side in range(4):
            at = place(side, t)
            lhs[s2:rows_all, at : at + LANES] = pro_raw[t, pl.ds(side, q2, stride=4), :].astype(
                jnp.bfloat16
            )

    rows_i = lax.broadcasted_iota(jnp.int32, (2 * LANES, 2 * LANES), 0)
    cols_i = lax.broadcasted_iota(jnp.int32, (2 * LANES, 2 * LANES), 1)
    wanted = jnp.where(rows_i < LANES, 2 * rows_i, 2 * (rows_i - LANES) + 1)
    chosen = jnp.where(cols_i == wanted, 1.0, 0.0).astype(jnp.bfloat16)
    corner_ends = (
        ((NORTH, 0), (WEST, 0)),
        ((NORTH, 1), (EAST, 0)),
        ((SOUTH, 0), (WEST, 1)),
        ((SOUTH, 1), (EAST, 1)),
    )
    for b in range(blocks):
        loads[b].wait()
        exact = dot(chosen, raw[2 * LANES * b : 2 * LANES * (b + 1)], ((1,), (0,)))
        row = place(b // thirds, b % thirds)
        picked = jnp.zeros((LANES, LANES), jnp.float32)
        for c in (0, 1):
            for j in (0, 1):
                for k in range(4):
                    side, end = corner_ends[k][j]
                    at = side * cells + end * (thirds - 1) * LANES
                    goal = c * 8 + j * 4 + k
                    moved = pltpu.roll(
                        exact[c * LANES : (c + 1) * LANES, at : at + LANES], (goal + end) % LANES, 1
                    )
                    picked = jnp.where(lane == goal, moved, picked)
        corner_table[row : row + LANES] = picked.astype(jnp.bfloat16)
        parted = exact.astype(jnp.bfloat16)
        for side in range(4):
            h, k = side // 2, 2 * (side % 2) * LANES
            for t in range(thirds):
                at = side * cells + t * LANES
                for c in (0, 1):
                    table[t, h, row : row + LANES, k + c * LANES : k + (c + 1) * LANES] = parted[
                        c * LANES : (c + 1) * LANES, at : at + LANES
                    ]

    def restrict(first, last):
        return restricted(out_hi[first:last], out_lo[first:last])

    def restricted(hi, lo):
        half = hi.shape[0] // 2
        both = dot(res_split[...], hi, ((1,), (1,)))
        rest = dot(res_split[0:q2], lo, ((1,), (1,)))
        u = both[0:q2] + both[q2:] + rest
        return u[0:half_q] + turned(u[half_q:], half)

    def coarse(total):
        stacked = jnp.concatenate([total, turned(total, half_s)], axis=0)
        coef = dot(inv_ref[...], stacked, ((0,), (0,)), HIGH)
        return coef

    def stack_of(coef):
        return jnp.concatenate([coef, turned(coef, half_s)], axis=0)

    def lifted(coef, k, first=0, last=depth):
        stack = stack_of(coef)
        hi = stack.astype(jnp.bfloat16)
        rest = (stack - hi.astype(jnp.float32)).astype(jnp.bfloat16)
        three = jnp.concatenate([hi, hi, rest], axis=0)
        fix[:, first:last] = dot(three, lift[k, :, first:last], ((0,), (0,)))

    def corner_columns(e):
        par, rows = e % 2, rows_of(e)
        for k in range(4):
            corner_copy(e, k).wait_recv()
        tile = []
        for base in (0, 4) if e <= 3 else (0,):
            for k in range(4):
                row = corner_in[par, k, base + 3 - k : base + 4 - k]
                tile.append(jnp.where(has_diag[k], 0.5 * row, 0.0))
        spare = jnp.zeros((LANES - len(tile), LANES), jnp.float32)
        flat = jnp.concatenate([*tile, spare], axis=0).T
        cols = flat[:, 0:4]
        if e <= 3:
            cols = jnp.concatenate([cols, flat[0:q2, 4:8]], axis=0)
        nw, ne, sw, se = (cols[:, k : k + 1] for k in range(4))
        return {NORTH: (nw, ne), SOUTH: (sw, se), WEST: (nw, sw), EAST: (ne, se)}

    def arrived(par, ends, side, t, first, last):
        value = jnp.where(has[side], got[par, side, t, first:last], 0.0)
        if t == 0:
            value += jnp.where(lane == 0, ends[side][0][first:last], 0.0)
        if t == thirds - 1:
            value += jnp.where(lane == LANES - 1, ends[side][1][first:last], 0.0)
        return value

    def receive_weights(ends):
        for t in order:
            for side in range(4):
                weight_copy(OUT_OF[side], t).wait_recv()
                at = place(side, t)
                extra = arrived(1, ends, side, t, s2, rows_all)
                hi = extra.astype(jnp.bfloat16)
                res_split[0:q2, at : at + LANES] = hi
                res_split[q2:, at : at + LANES] = (extra - hi.astype(jnp.float32)).astype(
                    jnp.bfloat16
                )
        for t in order:
            for side in range(4):
                weight_copy(side, t).wait_send()

    def receive(e, some, fixed, ends=None):
        par, rows = e % 2, rows_of(e)
        first, last = place(0, some[0]), place(0, some[-1]) + 4 * LANES
        ends = corner_columns(e) if ends is None else ends

        def incoming(side, t, first, last):
            return arrived(par, ends, side, t, first, last)

        for t in some:
            for side in range(4):
                side_copy(e, OUT_OF[side], t).wait_recv()
                if rows > s2:
                    at = place(side, t)
                    extra = incoming(side, t, s2, rows)
                    hi = extra.astype(jnp.bfloat16)
                    rest = (extra - hi.astype(jnp.float32)).astype(jnp.bfloat16)
                    lift[e - 2, 0:q2, at : at + LANES] = hi
                    lift[e - 2, q2 : 2 * q2, at : at + LANES] = rest
                    lift[e - 2, 2 * q2 :, at : at + LANES] = hi
                    if e == 2:
                        lhs[s2:, at : at + LANES] = hi
        if e == 3:
            lifted(fixed, 1, first, last)
        for t in some:
            for side in range(4):
                at = place(side, t)
                top = incoming(side, t, 0, s2)
                if fixed is not None:
                    top += fix[:, at : at + LANES]
                if e == ITERS:
                    last_sum[:, at : at + LANES] = top
                else:
                    lhs[0:s2, at : at + LANES] = top.astype(jnp.bfloat16)
        return ends

    def sends_done(e):
        for t in order:
            for side in range(4):
                side_copy(e, side, t).wait_send()
        for k in range(4):
            corner_copy(e, k).wait_send()

    def multiply_early(e):
        rows = rows_of(e)
        corner_acc[0:rows] = dot(lhs[0:rows, 0:early], corner_table[0:early], ((1,), (0,)))
        for t in order:
            for h in (0, 1):
                acc[t, h, 0:rows] = dot(lhs[0:rows, 0:early], table[t, h, 0:early], ((1,), (0,)))

    def multiply_late(e, sums):
        rows, par = rows_of(e), e % 2
        if e >= 3:
            sends_done(e - 2)

        z = corner_acc[0:rows] + dot(lhs[0:rows, early:], corner_table[early:], ((1,), (0,)))
        re = z + pltpu.roll(z, LANES - 4, 1)
        im = pltpu.roll(re, LANES - 8, 1)
        a, b = half_s, s2
        parts = [
            re[0:a] - im[a:b] + corner_src[0:a],
            im[0:a] + re[a:b] + corner_src[a:b],
        ]
        if rows > s2:
            a, b = s2 + half_q, s2 + q2
            parts += [re[s2:a] - im[a:b], im[s2:a] + re[a:b]]
        send_corners(e, jnp.concatenate(parts, axis=0))

        for t in order:
            if t == order[-1]:
                for a in sums:
                    sum_b(a)
            for h in (0, 1):
                product = acc[t, h, 0:rows] + dot(
                    lhs[0:rows, early:], table[t, h, early:], ((1,), (0,))
                )
                for k in (0, 1):
                    side = 2 * h + k
                    re = product[:, 2 * k * LANES : (2 * k + 1) * LANES]
                    im = product[:, (2 * k + 1) * LANES : (2 * k + 2) * LANES]
                    a, b = half_s, s2
                    out_re = re[0:a] - im[a:b] + src_ref[side, t, 0:a]
                    out_im = im[0:a] + re[a:b] + src_ref[side, t, a:b]
                    sent[par, side, t, 0:a] = out_re
                    sent[par, side, t, a:b] = out_im
                    if e < ITERS:
                        split(out_re, side, t, 0, a)
                        split(out_im, side, t, a, b)
                    if rows > s2:
                        a, b = s2 + half_q, s2 + q2
                        out_re = re[s2:a] - im[a:b]
                        out_im = im[s2:a] + re[a:b]
                        sent[par, side, t, s2:a] = out_re
                        sent[par, side, t, a:b] = out_im
                        split(out_re, side, t, s2, a)
                        split(out_im, side, t, a, b)
                    side_copy(e, side, t).start()

    coef, share = {}, {}

    def finish(j):
        total = sum_end(j)
        if j == 2:
            share[0] = sum_end(0)[:, 0:q2]
        if j == 3:
            share[1] = sum_end(ITERS)[:, 0:q2]
        for k in (0, 1):
            if j - 1 - k >= 1:
                total += dot(share[k], stack_of(coef[j - 1 - k]), ((1,), (0,)), HIGH)
        coef[j] = coarse(total)

    def lifted_rows():
        half = restrict(s2, rows_all)
        return jnp.concatenate([half, jnp.zeros((half_q, LANES - q2), jnp.float32)], axis=1)

    for i in range(1, ITERS):
        ends = receive(i, order[:-1], coef.get(i - 2))
        multiply_early(i + 1)
        if i == ITERS - 1:
            sum_b(i)
        if i >= 3:
            sum_c(i - 1)
        if i == 3:
            sum_c(0)
        if i == 4:
            sum_c(ITERS)
        receive(i, order[-1:], coef.get(i - 2), ends)
        if i == 1:
            receive_weights(ends)
            start_sum(1, restricted(src_hi[...], src_lo[...]))
        multiply_late(i + 1, {2: (2, 0), 3: (3, ITERS), 4: (4,)}.get(i, ()))
        if i == 2:
            sum_c(1)
        if i < ITERS - 1:
            start_sum(i + 1, restrict(0, s2))
        if i == 1:
            start_sum(0, lifted_rows())
            sum_b(1)
        if i == 2:
            start_sum(ITERS, lifted_rows())
            finish(1)
        if i >= 3:
            finish(i - 1)
            lifted(coef[i - 1], 1)
        if i == ITERS - 1:
            sum_c(i)

    ends = receive(ITERS, order[:-1], coef[ITERS - 2])
    receive(ITERS, order[-1:], coef[ITERS - 2], ends)
    finish(ITERS - 1)
    coef_ref[0] = coef[ITERS - 1][:, 0:half_s]
    coef_ref[1] = coef[ITERS - 1][:, half_s:]
    coef_store.start()
    lifted(coef[ITERS - 1], 0)
    flat_out = out_hbm.reshape(4 * s2, cells)
    stores = [
        pltpu.make_async_copy(
            src_raw.at[t], flat_out.at[:, pl.ds(t * LANES, LANES)], load_sem.at[0, t]
        )
        for t in range(thirds)
    ]
    for t in range(thirds):
        for side in range(4):
            at = place(side, t)
            src_raw[t, pl.ds(side, s2, stride=4), :] = (
                last_sum[:, at : at + LANES] + fix[:, at : at + LANES]
            )
        stores[t].start()
    sends_done(ITERS - 1)
    sends_done(ITERS)
    for a in range(ITERS + 1):
        for stage in range(3):
            whole(a, stage).wait_send()
    for t in range(thirds):
        stores[t].wait()
    coef_store.wait()


def solution(mesh):
    nsy, nz = mesh.shape["sy"], mesh.shape["sx"]
    nx = 4
    ny = nsy // nx

    def per_device(interface_map, source_trace, restriction, prolongation, coarse_inverse):
        src_count, cells = source_trace.shape[3], source_trace.shape[5]
        width = restriction.shape[3]
        thirds = cells // LANES
        s2, q2 = 2 * src_count, 2 * width
        rows = s2 + q2
        depth = 4 * cells
        dims = (ny, nx, nz, s2, q2, thirds)
        chunk = width // ny
        hbm = pl.BlockSpec(memory_space=pl.ANY)
        traces, coef = pl.pallas_call(
            functools.partial(kernel, dims),
            out_shape=(
                jax.ShapeDtypeStruct((2, src_count, 4, cells), jnp.float32),
                jax.ShapeDtypeStruct((2, width, src_count), jnp.float32),
            ),
            in_specs=[hbm] * 5,
            out_specs=(hbm, hbm),
            scratch_shapes=[
                pltpu.VMEM((q2, width), jnp.float32),
                pltpu.VMEM((2, width, src_count), jnp.float32),
                pltpu.VMEM((2 * depth, depth), jnp.bfloat16),
                pltpu.VMEM((thirds, 4 * s2, LANES), jnp.float32),
                pltpu.VMEM((thirds, 4 * q2, LANES), jnp.float32),
                pltpu.VMEM((thirds, 4 * q2, LANES), jnp.float32),
                pltpu.VMEM((4, thirds, s2, LANES), jnp.float32),
                pltpu.VMEM((thirds, 2, depth, 4 * LANES), jnp.bfloat16),
                pltpu.VMEM((rows, depth), jnp.bfloat16),
                pltpu.VMEM((thirds, 2, rows, 4 * LANES), jnp.float32),
                pltpu.VMEM((s2, depth), jnp.bfloat16),
                pltpu.VMEM((s2, depth), jnp.bfloat16),
                pltpu.VMEM((rows, depth), jnp.bfloat16),
                pltpu.VMEM((rows, depth), jnp.bfloat16),
                pltpu.VMEM((2, 4, thirds, rows, LANES), jnp.float32),
                pltpu.VMEM((2, 4, thirds, rows, LANES), jnp.float32),
                pltpu.VMEM((2, 3 * q2, depth), jnp.bfloat16),
                pltpu.VMEM((2 * q2, depth), jnp.bfloat16),
                pltpu.VMEM((depth, LANES), jnp.bfloat16),
                pltpu.VMEM((rows, LANES), jnp.float32),
                pltpu.VMEM((s2, LANES), jnp.float32),
                pltpu.VMEM((2, 8, LANES), jnp.float32),
                pltpu.VMEM((2, 4, 8, LANES), jnp.float32),
                pltpu.VMEM((ITERS + 1, ny, chunk, LANES), jnp.float32),
                pltpu.VMEM((ITERS + 1, nsy, chunk, LANES), jnp.float32),
                pltpu.VMEM((ITERS + 1, chunk, LANES), jnp.float32),
                pltpu.VMEM((ITERS + 1, nz, chunk, LANES), jnp.float32),
                pltpu.VMEM((ITERS + 1, chunk, LANES), jnp.float32),
                pltpu.VMEM((ITERS + 1, ny, chunk, LANES), jnp.float32),
                pltpu.VMEM((s2, depth), jnp.float32),
                pltpu.VMEM((s2, depth), jnp.float32),
                pltpu.SemaphoreType.DMA((depth // LANES,)),
                pltpu.SemaphoreType.DMA((3, thirds)),
                pltpu.SemaphoreType.DMA((2,)),
                pltpu.SemaphoreType.DMA((2, 4, thirds)),
                pltpu.SemaphoreType.DMA((2, 4, thirds)),
                pltpu.SemaphoreType.DMA((4, thirds)),
                pltpu.SemaphoreType.DMA((4, thirds)),
                pltpu.SemaphoreType.DMA((2, 4)),
                pltpu.SemaphoreType.DMA((2, 4)),
                pltpu.SemaphoreType.DMA((ITERS + 1, 3)),
                pltpu.SemaphoreType.DMA((ITERS + 1, 3)),
            ],
            compiler_params=pltpu.CompilerParams(
                collective_id=0, has_side_effects=True, vmem_limit_bytes=60 * 1024 * 1024
            ),
        )(
            interface_map.reshape(depth, 2, depth),
            source_trace.reshape(2, src_count, 4, cells),
            restriction.reshape(2, width, 4, cells),
            prolongation.reshape(2, width, 4, cells),
            coarse_inverse.reshape(q2, width),
        )
        return traces.reshape(source_trace.shape), coef.transpose(0, 2, 1)

    where = P(("wl", "sy"), "sx", None, None, None, None)
    return jax.shard_map(
        per_device,
        mesh=mesh,
        in_specs=(P(("wl", "sy"), "sx", None, None, None), where, where, where, P("wl", None, None)),
        out_specs=(where, P("wl", None, None)),
        check_vma=False,
    )
```

```python
import functools

import jax
import jax.numpy as jnp
from jax import lax
from jax.experimental import pallas as pl
from jax.experimental.pallas import tpu as pltpu
from jax.sharding import PartitionSpec as P

ITERS = 6
LANES = 128
MESH = pl.DeviceIdType.MESH
HIGH = lax.Precision.HIGHEST
NORTH, SOUTH, WEST, EAST = 0, 1, 2, 3
OUT_OF = {NORTH: SOUTH, SOUTH: NORTH, WEST: EAST, EAST: WEST}


def dot(a, b, contract, precision=None):
    return lax.dot_general(
        a, b, (contract, ((), ())), preferred_element_type=jnp.float32, precision=precision
    )


def turned(pair, half):
    return jnp.concatenate([-pair[:, half:], pair[:, :half]], axis=1)


def kernel(
    dims,
    map_hbm,
    src_hbm,
    res_hbm,
    pro_hbm,
    inv_hbm,
    out_hbm,
    coef_hbm,
    inv_ref,
    coef_ref,
    raw,
    src_raw,
    res_raw,
    pro_raw,
    src_ref,
    table,
    lhs,
    acc,
    src_hi,
    src_lo,
    out_hi,
    out_lo,
    sent,
    got,
    lift,
    res_split,
    corner_table,
    corner_acc,
    corner_src,
    corner_out,
    corner_in,
    part,
    plane_in,
    line_out,
    line_in,
    col_out,
    col_in,
    fix,
    last_sum,
    map_sem,
    load_sem,
    small_sem,
    send_sem,
    recv_sem,
    wsend_sem,
    wrecv_sem,
    csend_sem,
    crecv_sem,
    asend_sem,
    arecv_sem,
):
    ny, nx, nz, s2, q2, thirds = dims
    cells = thirds * LANES
    nsy = ny * nx
    rows_all = s2 + q2
    half_s, half_q = s2 // 2, q2 // 2
    sy, sx = lax.axis_index("sy"), lax.axis_index("sx")
    wl = lax.axis_index("wl")
    yy = sy // nx

    def dev(row, col):
        return (row, col, wl)

    def place(side, t):
        return (order.index(t) * 4 + side) * LANES

    up, down = lax.rem(sy + nsy - 1, nsy), lax.rem(sy + 1, nsy)
    left, right = lax.rem(sx + nz - 1, nz), lax.rem(sx + 1, nz)
    peer = {NORTH: dev(up, sx), SOUTH: dev(down, sx), WEST: dev(sy, left), EAST: dev(sy, right)}
    diag = (dev(up, left), dev(up, right), dev(down, left), dev(down, right))
    has = {NORTH: sy > 0, SOUTH: sy < nsy - 1, WEST: sx > 0, EAST: sx < nz - 1}
    has_diag = (
        (sy > 0) & (sx > 0),
        (sy > 0) & (sx < nz - 1),
        (sy < nsy - 1) & (sx > 0),
        (sy < nsy - 1) & (sx < nz - 1),
    )

    depth = 4 * cells
    order = (0, *range(2, thirds), 1)
    early = 4 * LANES * (thirds - 1)
    blocks = depth // LANES
    flat_map = map_hbm.reshape(2 * depth, depth)
    loads = [
        pltpu.make_async_copy(
            flat_map.at[pl.ds(2 * LANES * b, 2 * LANES)],
            raw.at[pl.ds(2 * LANES * b, 2 * LANES)],
            map_sem.at[b],
        )
        for b in range(blocks)
    ]
    flat_src = src_hbm.reshape(4 * s2, cells)
    flat_pro = pro_hbm.reshape(4 * q2, cells)
    flat_res = res_hbm.reshape(4 * q2, cells)

    def third(flat, held, which):
        return [
            pltpu.make_async_copy(
                flat.at[:, pl.ds(t * LANES, LANES)], held.at[t], load_sem.at[which, t]
            )
            for t in range(thirds)
        ]

    src_load = third(flat_src, src_raw, 0)
    pro_load = third(flat_pro, pro_raw, 1)
    res_load = third(flat_res, res_raw, 2)
    inv_load = pltpu.make_async_copy(inv_hbm, inv_ref, small_sem.at[0])
    coef_store = pltpu.make_async_copy(coef_ref, coef_hbm, small_sem.at[1])
    for copy in (*src_load, *res_load, *pro_load, inv_load):
        copy.start()
    for b in range(blocks):
        loads[b].start()

    barrier = pltpu.get_barrier_semaphore()
    met = 0
    for target in (*peer.values(), *diag):
        pl.semaphore_signal(barrier, inc=1, device_id=target, device_id_type=MESH)
        met += 1
    for d in range(1, nsy):
        target = dev(lax.rem(sy + d, nsy), sx)
        pl.semaphore_signal(barrier, inc=1, device_id=target, device_id_type=MESH)
        met += 1
    for d in range(1, nz):
        target = dev(sy, lax.rem(sx + d, nz))
        pl.semaphore_signal(barrier, inc=1, device_id=target, device_id_type=MESH)
        met += 1
    for t in order:
        src_load[t].wait()
        res_load[t].wait()
        for side in range(4):
            at = place(side, t)
            value = src_raw[t, pl.ds(side, s2, stride=4), :]
            src_ref[side, t] = value
            sent[1, side, t, 0:s2] = value
            sent[1, side, t, s2:] = res_raw[t, pl.ds(side, q2, stride=4), :]
    pl.semaphore_wait(barrier, met)

    lane = lax.broadcasted_iota(jnp.int32, (1, LANES), 1)

    def rows_of(e):
        return rows_all if e in (2, 3) else s2

    def side_copy(e, side, t):
        par, rows = e % 2, rows_of(e)
        return pltpu.make_async_remote_copy(
            src_ref=sent.at[par, side, t, pl.ds(0, rows)],
            dst_ref=got.at[par, OUT_OF[side], t, pl.ds(0, rows)],
            send_sem=send_sem.at[par, side, t],
            recv_sem=recv_sem.at[par, OUT_OF[side], t],
            device_id=peer[side],
            device_id_type=MESH,
        )

    def weight_copy(side, t):
        return pltpu.make_async_remote_copy(
            src_ref=sent.at[1, side, t, pl.ds(s2, q2)],
            dst_ref=got.at[1, OUT_OF[side], t, pl.ds(s2, q2)],
            send_sem=wsend_sem.at[side, t],
            recv_sem=wrecv_sem.at[OUT_OF[side], t],
            device_id=peer[side],
            device_id_type=MESH,
        )

    def corner_copy(e, k):
        par = e % 2
        return pltpu.make_async_remote_copy(
            src_ref=corner_out.at[par],
            dst_ref=corner_in.at[par, 3 - k],
            send_sem=csend_sem.at[par, k],
            recv_sem=crecv_sem.at[par, 3 - k],
            device_id=diag[k],
            device_id_type=MESH,
        )

    def source_corners(block):
        last = thirds - 1
        n0, n1 = block(NORTH, 0)[:, 0:1], block(NORTH, last)[:, LANES - 1 :]
        s0, s1 = block(SOUTH, 0)[:, 0:1], block(SOUTH, last)[:, LANES - 1 :]
        w0, w1 = block(WEST, 0)[:, 0:1], block(WEST, last)[:, LANES - 1 :]
        e0, e1 = block(EAST, 0)[:, 0:1], block(EAST, last)[:, LANES - 1 :]
        nw, ne, sw, se = n0 + w0, n1 + e0, s0 + w1, s1 + e1
        return jnp.where(
            lane == 0, nw, jnp.where(lane == 1, ne, jnp.where(lane == 2, sw, se))
        )

    def send_corners(e, z):
        first = z[0:LANES].T[0:4]
        if z.shape[0] > s2:
            spare = jnp.zeros((2 * LANES - z.shape[0], LANES), jnp.float32)
            second = jnp.concatenate([z[LANES:], spare], axis=0).T[0:4]
        else:
            second = jnp.zeros_like(first)
        corner_out[e % 2] = jnp.concatenate([first, second], axis=0)
        for k in range(4):
            corner_copy(e, k).start()

    chunk = part.shape[2]

    def stage_a(a, j):
        d = j
        target = lax.rem(sy + d, nsy)
        return pltpu.make_async_remote_copy(
            src_ref=part.at[a, target // nx],
            dst_ref=plane_in.at[a, nsy - d],
            send_sem=asend_sem.at[a, 0],
            recv_sem=arecv_sem.at[a, 0],
            device_id=dev(target, sx),
            device_id_type=MESH,
        )

    def stage_b(a, d):
        return pltpu.make_async_remote_copy(
            src_ref=line_out.at[a],
            dst_ref=line_in.at[a, nz - d],
            send_sem=asend_sem.at[a, 1],
            recv_sem=arecv_sem.at[a, 1],
            device_id=dev(sy, lax.rem(sx + d, nz)),
            device_id_type=MESH,
        )

    def stage_c(a, d):
        return pltpu.make_async_remote_copy(
            src_ref=col_out.at[a],
            dst_ref=col_in.at[a, ny - d],
            send_sem=asend_sem.at[a, 2],
            recv_sem=arecv_sem.at[a, 2],
            device_id=dev(lax.rem(sy + d * nx, nsy), sx),
            device_id_type=MESH,
        )

    def whole(a, stage):
        buf = (plane_in, line_in, col_in)[stage]
        n = (nsy, nz, ny)[stage]
        ref = buf.at[a, pl.ds(1, n - 1)]
        return pltpu.make_async_remote_copy(
            src_ref=ref,
            dst_ref=ref,
            send_sem=asend_sem.at[a, stage],
            recv_sem=arecv_sem.at[a, stage],
            device_id=peer[EAST],
            device_id_type=MESH,
        )

    def summed(values):
        while len(values) > 1:
            values = [
                values[i] + values[i + 1] if i + 1 < len(values) else values[i]
                for i in range(0, len(values), 2)
            ]
        return values[0]

    def start_sum(a, payload):
        for j in range(ny):
            part[a, j] = payload[j * chunk : (j + 1) * chunk]
        for d in range(1, nsy):
            stage_a(a, d).start()

    def sum_b(a):
        whole(a, 0).wait_recv()
        plane_in[a, 0] = part[a, yy]
        line_out[a] = summed([plane_in[a, lax.rem(j - sy + nsy, nsy)] for j in range(nsy)])
        for d in range(1, nz):
            stage_b(a, d).start()

    def sum_c(a):
        whole(a, 1).wait_recv()
        line_in[a, 0] = line_out[a]
        col_out[a] = summed([line_in[a, lax.rem(j - sx + nz, nz)] for j in range(nz)])
        for d in range(1, ny):
            stage_c(a, d).start()

    def sum_end(a):
        whole(a, 2).wait_recv()
        col_in[a, 0] = col_out[a]
        return jnp.concatenate([col_in[a, lax.rem(j - yy + ny, ny)] for j in range(ny)], axis=0)

    corners = source_corners(lambda side, t: sent[1, side, t])
    corner_src[...] = corners[0:s2]
    send_corners(1, corners)
    for t in order:
        for side in range(4):
            side_copy(1, side, t).start()
    for t in order:
        for side in range(4):
            weight_copy(side, t).start()

    def split(value, side, t, first, last):
        at = place(side, t)
        hi = value.astype(jnp.bfloat16)
        out_hi[first:last, at : at + LANES] = hi
        out_lo[first:last, at : at + LANES] = (value - hi.astype(jnp.float32)).astype(jnp.bfloat16)

    for t in order:
        for side in range(4):
            at, value = place(side, t), src_ref[side, t]
            hi = value.astype(jnp.bfloat16)
            src_hi[:, at : at + LANES] = hi
            src_lo[:, at : at + LANES] = (value - hi.astype(jnp.float32)).astype(jnp.bfloat16)

    inv_load.wait()
    for t in order:
        pro_load[t].wait()
        for side in range(4):
            at = place(side, t)
            lhs[s2:rows_all, at : at + LANES] = pro_raw[t, pl.ds(side, q2, stride=4), :].astype(
                jnp.bfloat16
            )

    rows_i = lax.broadcasted_iota(jnp.int32, (2 * LANES, 2 * LANES), 0)
    cols_i = lax.broadcasted_iota(jnp.int32, (2 * LANES, 2 * LANES), 1)
    wanted = jnp.where(rows_i < LANES, 2 * rows_i, 2 * (rows_i - LANES) + 1)
    chosen = jnp.where(cols_i == wanted, 1.0, 0.0).astype(jnp.bfloat16)
    corner_ends = (
        ((NORTH, 0), (WEST, 0)),
        ((NORTH, 1), (EAST, 0)),
        ((SOUTH, 0), (WEST, 1)),
        ((SOUTH, 1), (EAST, 1)),
    )
    for b in range(blocks):
        loads[b].wait()
        exact = dot(chosen, raw[2 * LANES * b : 2 * LANES * (b + 1)], ((1,), (0,)))
        row = place(b // thirds, b % thirds)
        picked = jnp.zeros((LANES, LANES), jnp.float32)
        for c in (0, 1):
            for j in (0, 1):
                for k in range(4):
                    side, end = corner_ends[k][j]
                    at = side * cells + end * (thirds - 1) * LANES
                    goal = c * 8 + j * 4 + k
                    moved = pltpu.roll(
                        exact[c * LANES : (c + 1) * LANES, at : at + LANES], (goal + end) % LANES, 1
                    )
                    picked = jnp.where(lane == goal, moved, picked)
        corner_table[row : row + LANES] = picked.astype(jnp.bfloat16)
        parted = exact.astype(jnp.bfloat16)
        for side in range(4):
            h, k = side // 2, 2 * (side % 2) * LANES
            for t in range(thirds):
                at = side * cells + t * LANES
                for c in (0, 1):
                    table[t, h, row : row + LANES, k + c * LANES : k + (c + 1) * LANES] = parted[
                        c * LANES : (c + 1) * LANES, at : at + LANES
                    ]

    def restrict(first, last):
        return restricted(out_hi[first:last], out_lo[first:last])

    def restricted(hi, lo):
        half = hi.shape[0] // 2
        both = dot(res_split[...], hi, ((1,), (1,)))
        rest = dot(res_split[0:q2], lo, ((1,), (1,)))
        u = both[0:q2] + both[q2:] + rest
        return u[0:half_q] + turned(u[half_q:], half)

    def coarse(total):
        stacked = jnp.concatenate([total, turned(total, half_s)], axis=0)
        coef = dot(inv_ref[...], stacked, ((0,), (0,)), HIGH)
        return coef

    def stack_of(coef):
        return jnp.concatenate([coef, turned(coef, half_s)], axis=0)

    def lifted(coef, k, first=0, last=depth):
        stack = stack_of(coef)
        hi = stack.astype(jnp.bfloat16)
        rest = (stack - hi.astype(jnp.float32)).astype(jnp.bfloat16)
        three = jnp.concatenate([hi, hi, rest], axis=0)
        fix[:, first:last] = dot(three, lift[k, :, first:last], ((0,), (0,)))

    def corner_columns(e):
        par, rows = e % 2, rows_of(e)
        for k in range(4):
            corner_copy(e, k).wait_recv()
        tile = []
        for base in (0, 4) if e <= 3 else (0,):
            for k in range(4):
                row = corner_in[par, k, base + 3 - k : base + 4 - k]
                tile.append(jnp.where(has_diag[k], 0.5 * row, 0.0))
        spare = jnp.zeros((LANES - len(tile), LANES), jnp.float32)
        flat = jnp.concatenate([*tile, spare], axis=0).T
        cols = flat[:, 0:4]
        if e <= 3:
            cols = jnp.concatenate([cols, flat[0:q2, 4:8]], axis=0)
        nw, ne, sw, se = (cols[:, k : k + 1] for k in range(4))
        return {NORTH: (nw, ne), SOUTH: (sw, se), WEST: (nw, sw), EAST: (ne, se)}

    def arrived(par, ends, side, t, first, last):
        value = jnp.where(has[side], got[par, side, t, first:last], 0.0)
        if t == 0:
            value += jnp.where(lane == 0, ends[side][0][first:last], 0.0)
        if t == thirds - 1:
            value += jnp.where(lane == LANES - 1, ends[side][1][first:last], 0.0)
        return value

    def receive_weights(ends):
        for t in order:
            for side in range(4):
                weight_copy(OUT_OF[side], t).wait_recv()
                at = place(side, t)
                extra = arrived(1, ends, side, t, s2, rows_all)
                hi = extra.astype(jnp.bfloat16)
                res_split[0:q2, at : at + LANES] = hi
                res_split[q2:, at : at + LANES] = (extra - hi.astype(jnp.float32)).astype(
                    jnp.bfloat16
                )
        for t in order:
            for side in range(4):
                weight_copy(side, t).wait_send()

    def receive(e, some, fixed, ends=None):
        par, rows = e % 2, rows_of(e)
        first, last = place(0, some[0]), place(0, some[-1]) + 4 * LANES
        ends = corner_columns(e) if ends is None else ends

        def incoming(side, t, first, last):
            return arrived(par, ends, side, t, first, last)

        for t in some:
            for side in range(4):
                side_copy(e, OUT_OF[side], t).wait_recv()
                if rows > s2:
                    at = place(side, t)
                    extra = incoming(side, t, s2, rows)
                    hi = extra.astype(jnp.bfloat16)
                    rest = (extra - hi.astype(jnp.float32)).astype(jnp.bfloat16)
                    lift[e - 2, 0:q2, at : at + LANES] = hi
                    lift[e - 2, q2 : 2 * q2, at : at + LANES] = rest
                    lift[e - 2, 2 * q2 :, at : at + LANES] = hi
                    if e == 2:
                        lhs[s2:, at : at + LANES] = hi
        if e == 3:
            lifted(fixed, 1, first, last)
        for t in some:
            for side in range(4):
                at = place(side, t)
                top = incoming(side, t, 0, s2)
                if fixed is not None:
                    top += fix[:, at : at + LANES]
                if e == ITERS:
                    last_sum[:, at : at + LANES] = top
                else:
                    lhs[0:s2, at : at + LANES] = top.astype(jnp.bfloat16)
        return ends

    def sends_done(e):
        for t in order:
            for side in range(4):
                side_copy(e, side, t).wait_send()
        for k in range(4):
            corner_copy(e, k).wait_send()

    def multiply_early(e):
        rows = rows_of(e)
        corner_acc[0:rows] = dot(lhs[0:rows, 0:early], corner_table[0:early], ((1,), (0,)))
        for t in order:
            for h in (0, 1):
                acc[t, h, 0:rows] = dot(lhs[0:rows, 0:early], table[t, h, 0:early], ((1,), (0,)))

    def multiply_late(e, sums):
        rows, par = rows_of(e), e % 2
        if e >= 3:
            sends_done(e - 2)

        z = corner_acc[0:rows] + dot(lhs[0:rows, early:], corner_table[early:], ((1,), (0,)))
        re = z + pltpu.roll(z, LANES - 4, 1)
        im = pltpu.roll(re, LANES - 8, 1)
        a, b = half_s, s2
        parts = [
            re[0:a] - im[a:b] + corner_src[0:a],
            im[0:a] + re[a:b] + corner_src[a:b],
        ]
        if rows > s2:
            a, b = s2 + half_q, s2 + q2
            parts += [re[s2:a] - im[a:b], im[s2:a] + re[a:b]]
        send_corners(e, jnp.concatenate(parts, axis=0))

        for t in order:
            if t == order[-1]:
                for a in sums:
                    sum_b(a)
            for h in (0, 1):
                product = acc[t, h, 0:rows] + dot(
                    lhs[0:rows, early:], table[t, h, early:], ((1,), (0,))
                )
                for k in (0, 1):
                    side = 2 * h + k
                    re = product[:, 2 * k * LANES : (2 * k + 1) * LANES]
                    im = product[:, (2 * k + 1) * LANES : (2 * k + 2) * LANES]
                    a, b = half_s, s2
                    out_re = re[0:a] - im[a:b] + src_ref[side, t, 0:a]
                    out_im = im[0:a] + re[a:b] + src_ref[side, t, a:b]
                    sent[par, side, t, 0:a] = out_re
                    sent[par, side, t, a:b] = out_im
                    if e < ITERS:
                        split(out_re, side, t, 0, a)
                        split(out_im, side, t, a, b)
                    if rows > s2:
                        a, b = s2 + half_q, s2 + q2
                        out_re = re[s2:a] - im[a:b]
                        out_im = im[s2:a] + re[a:b]
                        sent[par, side, t, s2:a] = out_re
                        sent[par, side, t, a:b] = out_im
                        split(out_re, side, t, s2, a)
                        split(out_im, side, t, a, b)
                    side_copy(e, side, t).start()

    coef, share = {}, {}

    def finish(j):
        total = sum_end(j)
        if j == 2:
            share[0] = sum_end(0)[:, 0:q2]
        if j == 3:
            share[1] = sum_end(ITERS)[:, 0:q2]
        for k in (0, 1):
            if j - 1 - k >= 1:
                total += dot(share[k], stack_of(coef[j - 1 - k]), ((1,), (0,)), HIGH)
        coef[j] = coarse(total)

    def lifted_rows():
        half = restrict(s2, rows_all)
        return jnp.concatenate([half, jnp.zeros((half_q, LANES - q2), jnp.float32)], axis=1)

    for i in range(1, ITERS):
        ends = receive(i, order[:-1], coef.get(i - 2))
        multiply_early(i + 1)
        if i == ITERS - 1:
            sum_b(i)
        if i >= 3:
            sum_c(i - 1)
        if i == 3:
            sum_c(0)
        if i == 4:
            sum_c(ITERS)
        receive(i, order[-1:], coef.get(i - 2), ends)
        if i == 1:
            receive_weights(ends)
            start_sum(1, restricted(src_hi[...], src_lo[...]))
        multiply_late(i + 1, {2: (2, 0), 3: (3, ITERS), 4: (4,)}.get(i, ()))
        if i == 2:
            sum_c(1)
        if i < ITERS - 1:
            start_sum(i + 1, restrict(0, s2))
        if i == 1:
            start_sum(0, lifted_rows())
            sum_b(1)
        if i == 2:
            start_sum(ITERS, lifted_rows())
            finish(1)
        if i >= 3:
            finish(i - 1)
            lifted(coef[i - 1], 1)
        if i == ITERS - 1:
            sum_c(i)

    ends = receive(ITERS, order[:-1], coef[ITERS - 2])
    receive(ITERS, order[-1:], coef[ITERS - 2], ends)
    finish(ITERS - 1)
    coef_ref[0] = coef[ITERS - 1][:, 0:half_s]
    coef_ref[1] = coef[ITERS - 1][:, half_s:]
    coef_store.start()
    lifted(coef[ITERS - 1], 0)
    flat_out = out_hbm.reshape(4 * s2, cells)
    stores = [
        pltpu.make_async_copy(
            src_raw.at[t], flat_out.at[:, pl.ds(t * LANES, LANES)], load_sem.at[0, t]
        )
        for t in range(thirds)
    ]
    for t in range(thirds):
        for side in range(4):
            at = place(side, t)
            src_raw[t, pl.ds(side, s2, stride=4), :] = (
                last_sum[:, at : at + LANES] + fix[:, at : at + LANES]
            )
        stores[t].start()
    sends_done(ITERS - 1)
    sends_done(ITERS)
    for a in range(ITERS + 1):
        for stage in range(3):
            whole(a, stage).wait_send()
    for t in range(thirds):
        stores[t].wait()
    coef_store.wait()


def hand_over(traces_hbm, coef_hbm, out_hbm, coef_out_hbm, traces, coef, in_sem, out_sem):
    halves, sources = traces.shape[0], traces.shape[1] // 2
    pieces = [(c, pl.ds(k * sources, sources)) for c in range(halves) for k in (0, 1)]
    moves = [
        (
            pltpu.make_async_copy(traces_hbm.at[c, d], traces.at[c, d], in_sem.at[n]),
            pltpu.make_async_copy(traces.at[c, d], out_hbm.at[c, d], out_sem.at[n]),
        )
        for n, (c, d) in enumerate(pieces)
    ]
    n = len(pieces)
    moves.append(
        (
            pltpu.make_async_copy(coef_hbm, coef, in_sem.at[n]),
            pltpu.make_async_copy(coef, coef_out_hbm, out_sem.at[n]),
        )
    )
    for load, _ in moves:
        load.start()
    for load, store in moves:
        load.wait()
        store.start()
    for _, store in moves:
        store.wait()


def solution(mesh):
    nsy, nz = mesh.shape["sy"], mesh.shape["sx"]
    nx = 4
    ny = nsy // nx

    def per_device(interface_map, source_trace, restriction, prolongation, coarse_inverse):
        src_count, cells = source_trace.shape[3], source_trace.shape[5]
        width = restriction.shape[3]
        thirds = cells // LANES
        s2, q2 = 2 * src_count, 2 * width
        rows = s2 + q2
        depth = 4 * cells
        dims = (ny, nx, nz, s2, q2, thirds)
        chunk = width // ny
        hbm = pl.BlockSpec(memory_space=pl.ANY)
        traces, coef = pl.pallas_call(
            functools.partial(kernel, dims),
            out_shape=(
                jax.ShapeDtypeStruct((2, src_count, 4, cells), jnp.float32),
                jax.ShapeDtypeStruct((2, width, src_count), jnp.float32),
            ),
            in_specs=[hbm] * 5,
            out_specs=(hbm, hbm),
            scratch_shapes=[
                pltpu.VMEM((q2, width), jnp.float32),
                pltpu.VMEM((2, width, src_count), jnp.float32),
                pltpu.VMEM((2 * depth, depth), jnp.bfloat16),
                pltpu.VMEM((thirds, 4 * s2, LANES), jnp.float32),
                pltpu.VMEM((thirds, 4 * q2, LANES), jnp.float32),
                pltpu.VMEM((thirds, 4 * q2, LANES), jnp.float32),
                pltpu.VMEM((4, thirds, s2, LANES), jnp.float32),
                pltpu.VMEM((thirds, 2, depth, 4 * LANES), jnp.bfloat16),
                pltpu.VMEM((rows, depth), jnp.bfloat16),
                pltpu.VMEM((thirds, 2, rows, 4 * LANES), jnp.float32),
                pltpu.VMEM((s2, depth), jnp.bfloat16),
                pltpu.VMEM((s2, depth), jnp.bfloat16),
                pltpu.VMEM((rows, depth), jnp.bfloat16),
                pltpu.VMEM((rows, depth), jnp.bfloat16),
                pltpu.VMEM((2, 4, thirds, rows, LANES), jnp.float32),
                pltpu.VMEM((2, 4, thirds, rows, LANES), jnp.float32),
                pltpu.VMEM((2, 3 * q2, depth), jnp.bfloat16),
                pltpu.VMEM((2 * q2, depth), jnp.bfloat16),
                pltpu.VMEM((depth, LANES), jnp.bfloat16),
                pltpu.VMEM((rows, LANES), jnp.float32),
                pltpu.VMEM((s2, LANES), jnp.float32),
                pltpu.VMEM((2, 8, LANES), jnp.float32),
                pltpu.VMEM((2, 4, 8, LANES), jnp.float32),
                pltpu.VMEM((ITERS + 1, ny, chunk, LANES), jnp.float32),
                pltpu.VMEM((ITERS + 1, nsy, chunk, LANES), jnp.float32),
                pltpu.VMEM((ITERS + 1, chunk, LANES), jnp.float32),
                pltpu.VMEM((ITERS + 1, nz, chunk, LANES), jnp.float32),
                pltpu.VMEM((ITERS + 1, chunk, LANES), jnp.float32),
                pltpu.VMEM((ITERS + 1, ny, chunk, LANES), jnp.float32),
                pltpu.VMEM((s2, depth), jnp.float32),
                pltpu.VMEM((s2, depth), jnp.float32),
                pltpu.SemaphoreType.DMA((depth // LANES,)),
                pltpu.SemaphoreType.DMA((3, thirds)),
                pltpu.SemaphoreType.DMA((2,)),
                pltpu.SemaphoreType.DMA((2, 4, thirds)),
                pltpu.SemaphoreType.DMA((2, 4, thirds)),
                pltpu.SemaphoreType.DMA((4, thirds)),
                pltpu.SemaphoreType.DMA((4, thirds)),
                pltpu.SemaphoreType.DMA((2, 4)),
                pltpu.SemaphoreType.DMA((2, 4)),
                pltpu.SemaphoreType.DMA((ITERS + 1, 3)),
                pltpu.SemaphoreType.DMA((ITERS + 1, 3)),
            ],
            compiler_params=pltpu.CompilerParams(
                collective_id=0, has_side_effects=True, vmem_limit_bytes=60 * 1024 * 1024
            ),
        )(
            interface_map.reshape(depth, 2, depth),
            source_trace.reshape(2, src_count, 4, cells),
            restriction.reshape(2, width, 4, cells),
            prolongation.reshape(2, width, 4, cells),
            coarse_inverse.reshape(q2, width),
        )
        traces, coef = pl.pallas_call(
            hand_over,
            out_shape=(
                jax.ShapeDtypeStruct(traces.shape, traces.dtype),
                jax.ShapeDtypeStruct(coef.shape, coef.dtype),
            ),
            in_specs=[hbm, hbm],
            out_specs=(hbm, hbm),
            scratch_shapes=[
                pltpu.VMEM(traces.shape, traces.dtype),
                pltpu.VMEM(coef.shape, coef.dtype),
                pltpu.SemaphoreType.DMA((5,)),
                pltpu.SemaphoreType.DMA((5,)),
            ],
        )(traces, coef)
        return traces.reshape(source_trace.shape), coef.transpose(0, 2, 1)

    where = P(("wl", "sy"), "sx", None, None, None, None)
    return jax.shard_map(
        per_device,
        mesh=mesh,
        in_specs=(P(("wl", "sy"), "sx", None, None, None), where, where, where, P("wl", None, None)),
        out_specs=(where, P("wl", None, None)),
        check_vma=False,
    )
```
